256 devices in a mesh: dp: 32 (over z_lo, x, core), feat: 8 (over y, z_hi).
Axes of the slice: x: 4, y: 4, z: 8 (z_hi: 2, z_lo: 4; z = z_hi * 4 + z_lo), core: 2. Of those that a mesh axis runs over, the one named last changes fastest.
Arguments:
- view_a: bfloat16 [4096, 4096], P('dp', 'feat'), may hold values from -24 to 24
- view_b: bfloat16 [4096, 4096], P('dp', 'feat'), may hold values from -24 to 24
Outputs:
- grad_a: bfloat16 [4096, 4096], P('dp', 'feat')
- grad_b: bfloat16 [4096, 4096], P('dp', 'feat')
- loss: float32 [], replicated
The draws below stay inside these ranges and needn't reach their ends.
All inputs are finite; a program needn't handle non-finite values.
Results may differ from the reference program's by a relative error of at most 0.0068.
Values may be sent and summed in bfloat16 or wider, within the bound.
A program may use at most 64 MiB of HBM per device.

```python
import math
import jax
import jax.numpy as jnp
from jax import lax

F = 4096
SAMPLES = 4096


def draw_pair(key):
    factors = max(F // 32, 4)
    own = jax.random.normal(jax.random.fold_in(key, 101), (SAMPLES, F), jnp.float32)
    loads = jax.random.normal(jax.random.fold_in(key, 102), (SAMPLES, factors), jnp.float32)
    mixing = jax.random.normal(jax.random.fold_in(key, 103), (factors, F), jnp.float32) / math.sqrt(factors)
    shared = jnp.dot(loads, mixing, precision=lax.Precision.HIGHEST)
    core_a = math.sqrt(0.5) * own + math.sqrt(0.5) * shared
    coupling = jax.random.uniform(jax.random.fold_in(key, 104), (F,), jnp.float32, 0.6, 0.95)
    noise = jax.random.normal(jax.random.fold_in(key, 105), (SAMPLES, F), jnp.float32)
    core_b = coupling * core_a + jnp.sqrt(1.0 - coupling * coupling) * noise
    first = jnp.clip(core_a, -8.0, 8.0)
    second = jnp.clip(core_b, -8.0, 8.0)
    return (first, second)


def draw_view_a(key, part):
    return draw_pair(key)[0].astype(jnp.bfloat16)


def draw_view_b(key, part):
    return draw_pair(key)[1].astype(jnp.bfloat16)


def setup_inputs(seed: int = 0) -> dict:
    streams_of = jax.random.split(jax.random.key(seed), 3)
    return {
        "view_a": draw_view_a(jax.random.fold_in(streams_of[2], 71), 0),
        "view_b": draw_view_b(jax.random.fold_in(streams_of[2], 71), 0),
    }


EPS = 1e-05
LAMBDA = 0.0051

def normalize(view):
    values = view.astype(jnp.float32)
    center = lax.optimization_barrier(jnp.mean(values, axis=0))
    spread = lax.optimization_barrier(jnp.mean(values * values, axis=0)) - center * center
    inverse = lax.rsqrt(spread + EPS)
    return ((values - center) * inverse, inverse)

def backward(grad, normed, inverse):
    first = lax.optimization_barrier(jnp.mean(grad, axis=0))
    second = lax.optimization_barrier(jnp.mean(grad * normed, axis=0))
    return (inverse * (grad - first - normed * second)).astype(jnp.bfloat16)

def reference(view_a, view_b):
    normed_a, inverse_a = normalize(view_a)
    normed_b, inverse_b = normalize(view_b)
    a_half = normed_a.astype(jnp.bfloat16)
    b_half = normed_b.astype(jnp.bfloat16)
    corr_t = jnp.dot(b_half.T, a_half, preferred_element_type=jnp.float32) / SAMPLES
    unit = jnp.eye(F, dtype=jnp.float32)
    total = jnp.sum(unit * (1.0 - corr_t) ** 2) + LAMBDA * jnp.sum((1.0 - unit) * corr_t * corr_t)
    loss = total / F
    grad_t = (unit * (-2.0 * (1.0 - corr_t)) + (1.0 - unit) * (2.0 * LAMBDA) * corr_t).astype(jnp.bfloat16)
    grad_na = jnp.dot(b_half, grad_t, preferred_element_type=jnp.float32)
    grad_nb = jnp.dot(a_half, grad_t.T, preferred_element_type=jnp.float32)
    return (backward(grad_na, normed_a, inverse_a), backward(grad_nb, normed_b, inverse_b), loss)
```

```python
import jax
import jax.numpy as jnp
from jax import lax
from jax.experimental import pallas as pl
from jax.experimental.pallas import tpu as pltpu
from jax.sharding import PartitionSpec as P

F = 4096
S = 4096
EPS = 1e-05
LAMBDA = 0.0051
MESH = pl.DeviceIdType.MESH
BF = jnp.bfloat16
F32 = jnp.float32


class Slots:
    def __init__(self):
        self.used = 0

    def take(self, n):
        first = self.used
        self.used += n
        return first


SEM = Slots()
I_V0 = SEM.take(1)
I_VZ = SEM.take(3)
I_XP, I_XM, I_XPF, I_XMF = (SEM.take(4) for _ in range(4))
I_W1 = SEM.take(2)
I_YP, I_YM, I_YPF, I_YMF = (SEM.take(2) for _ in range(4))
I_WD = SEM.take(8)
I_DA, I_DB, I_DZ = (SEM.take(1) for _ in range(3))
I_DY = SEM.take(3)
I_P1P, I_P1M = (SEM.take(4) for _ in range(2))
I_P2P, I_P2M = (SEM.take(8) for _ in range(2))
I_OZ = SEM.take(3)
I_OD = SEM.take(1)
I_GD = SEM.take(4)
I_Y1P, I_Y1M = (SEM.take(2) for _ in range(2))
I_Y2P, I_Y2M = (SEM.take(4) for _ in range(2))
I_A2 = SEM.take(2)
N_SEM = SEM.used


def kernel(
    a_in, b_in, ga_out, gb_out, loss_out,
    va, vbt, bt_loc, asum, asq, bsum, bsq, raw, g1, g2, rowv, colv,
    dtile, darr, dsum, dboth, ltile, lz, lzsum, ly,
    p1p_s, p1m_s, p1p_r, p1m_r, aug, p2p_s, p2m_s, p2p_r, p2m_r, ga_own,
    oz_s, oz_r, od_s, gfa,
    gd_s, gd_r, gb_own, y1p_s, y1m_s, y1p_r, y1m_r, y2p_s, y2m_s, y2p_r, y2m_r,
    a2_s, gfin, ssem, rsem,
):
    dp = lax.axis_index("dp")
    ft = lax.axis_index("feat")
    r, k = lax.div(dp, 2), lax.rem(dp, 2)
    zl, x = lax.div(r, 4), lax.rem(r, 4)
    y, zh = lax.div(ft, 2), lax.rem(ft, 2)
    o = 1 - k
    xp, x2, xm = lax.rem(x + 1, 4), lax.rem(x + 2, 4), lax.rem(x + 3, 4)
    yp, y2, ym = lax.rem(y + 1, 4), lax.rem(y + 2, 4), lax.rem(y + 3, 4)
    zq = (zl, zl + 1 - 2 * lax.rem(zl, 2), lax.rem(zl + 2, 4), 3 - zl)
    zhs = (zh, 1 - zh)

    def dev(r_, k_, f_):
        return (r_ * 2 + k_, f_)

    def rc(src, dst, i, to):
        return pltpu.make_async_remote_copy(
            src_ref=src, dst_ref=dst, send_sem=ssem.at[i], recv_sem=rsem.at[i],
            device_id=to, device_id_type=MESH,
        )

    def lanes(i, n):
        return pl.ds(pl.multiple_of(i * n, n), n)

    to_xp, to_xm = dev(zl * 4 + xp, k, ft), dev(zl * 4 + xm, k, ft)
    to_yp, to_ym = dev(r, k, yp * 2 + zh), dev(r, k, ym * 2 + zh)
    partner = dev(r, o, ft)

    barrier = pltpu.get_barrier_semaphore()

    def greet(to):
        pl.semaphore_signal(barrier, inc=1, device_id=to, device_id_type=MESH)

    greet(partner)
    for f_ in (yp, y2, ym):
        greet(dev(r, k, f_ * 2 + zh))

    @pl.loop(1, 16)
    def _(t):
        greet(dev(lax.rem(r + t, 16), k, ft))

    @pl.loop(0, 16)
    def _(t):
        greet(dev(lax.rem(r + t, 16), k, y * 2 + zhs[1]))

    for c in range(4):
        bt_loc[c * 128:(c + 1) * 128, :] = (
            b_in[:, c * 128:(c + 1) * 128].astype(F32).T.astype(BF)
        )
    va[k, r] = a_in[:, lanes(k, 256)]
    vbt[k, ft, :, lanes(r, 128)] = bt_loc[lanes(r, 32), :]
    pl.semaphore_wait(barrier, 35)

    c_v0 = rc(a_in.at[:, lanes(o, 256)], va.at[k, r], I_V0, partner)
    c_v0.start()

    def c_w1(t, h):
        to = lax.rem(r + t, 16)
        return rc(
            bt_loc.at[lanes(to, 32), :], vbt.at[k, ft, :, lanes(r, 128)],
            I_W1 + h, dev(to, k, y * 2 + zhs[h]),
        )

    @pl.loop(0, 16)
    def _(t):
        c_w1(t, 1).start()

    @pl.loop(1, 16)
    def _(t):
        c_w1(t, 0).start()

    w1_all = (
        rc(vbt.at[k, ft, :, 0:1920], vbt.at[k, ft, :, 0:1920], I_W1, partner),
        rc(vbt.at[k, y * 2 + zhs[1]], vbt.at[k, y * 2 + zhs[1]], I_W1 + 1, partner),
    )

    def c_vz(q):
        return rc(va.at[:, r], va.at[:, r], I_VZ + q - 1, dev(zq[q] * 4 + x, k, ft))

    def c_xp(q):
        s = zq[q] * 4 + x
        return rc(va.at[:, s], va.at[:, s], I_XP + q, to_xp)

    def c_xm(q):
        s = zq[q] * 4 + x
        return rc(va.at[:, s], va.at[:, s], I_XM + q, to_xm)

    def c_xpf(q):
        s = zq[q] * 4 + xm
        return rc(va.at[0, s], va.at[0, s], I_XPF + q, to_xp)

    def c_xmf(q):
        s = zq[q] * 4 + xp
        return rc(va.at[1, s], va.at[1, s], I_XMF + q, to_xm)

    def c_yp(h):
        s = y * 2 + zhs[h]
        return rc(vbt.at[k, s], vbt.at[k, s], I_YP + h, to_yp)

    def c_ym(h):
        s = y * 2 + zhs[h]
        return rc(vbt.at[k, s], vbt.at[k, s], I_YM + h, to_ym)

    def c_ypf(h):
        s = ym * 2 + zhs[h]
        return rc(vbt.at[k, s, 0:16], vbt.at[k, s, 0:16], I_YPF + h, to_yp)

    def c_ymf(h):
        s = yp * 2 + zhs[h]
        return rc(vbt.at[k, s, 16:32], vbt.at[k, s, 16:32], I_YMF + h, to_ym)

    def c_wd(j, h):
        s = (y, ym, yp, y2)[j] * 2 + zhs[h]
        return rc(vbt.at[k, s], vbt.at[k, s], I_WD + j * 2 + h, partner)

    c_v0.wait_recv()
    c_xp(0).start()
    c_xm(0).start()
    for q in (1, 2, 3):
        c_vz(q).start()
    for h in (0, 1):
        w1_all[h].wait_recv()
        c_yp(h).start()
        c_ym(h).start()
        c_wd(0, h).start()

    def x_next(q):
        c_vz(q).wait_recv()
        c_xp(q).start()
        c_xm(q).start()

    def x_forward(q):
        c_xp(q).wait_recv()
        c_xpf(q).start()
        c_xm(q).wait_recv()
        c_xmf(q).start()

    def y_forward(h):
        c_yp(h).wait_recv()
        c_ypf(h).start()
        c_wd(1, h).start()
        c_ym(h).wait_recv()
        c_ymf(h).start()
        c_wd(2, h).start()

    def y_last(h):
        c_ypf(h).wait_recv()
        c_ymf(h).wait_recv()
        c_wd(3, h).start()

    x_next(1)
    x_forward(0)
    y_forward(0)
    x_next(2)
    x_forward(1)
    y_forward(1)
    x_next(3)
    x_forward(2)
    y_last(0)
    x_forward(3)
    y_last(1)
    for q in range(4):
        c_xpf(q).wait_recv()
        c_xmf(q).wait_recv()
    for h in (0, 1):
        for j in range(4):
            c_wd(j, h).wait_recv()

    asum[...] = jnp.zeros_like(asum)
    asq[...] = jnp.zeros_like(asq)
    bsum[...] = jnp.zeros_like(bsum)
    bsq[...] = jnp.zeros_like(bsq)

    for kk in range(2):
        @pl.loop(0, 16)
        def _(c):
            blk = va[kk, c].astype(F32).reshape(16, 8, 256)
            asum[...] += jnp.sum(blk, axis=0)
            asq[...] += jnp.sum(blk * blk, axis=0)
            bl = vbt[kk, :, :, lanes(c, 128)].astype(F32).reshape(256, 128)
            bsum[...] += bl
            bsq[...] += bl * bl

    raw[...] = jnp.zeros_like(raw)
    for kk in range(2):
        @pl.loop(0, 4)
        def _(c):
            raw[...] += jnp.dot(
                vbt[kk, :, :, lanes(c, 512)].reshape(256, 512),
                va[kk, pl.ds(c * 4, 4)].reshape(512, 256),
                preferred_element_type=F32,
            )

    ma = jnp.sum(asum[...], axis=0, keepdims=True) / S
    inva = lax.rsqrt(jnp.sum(asq[...], axis=0, keepdims=True) / S - ma * ma + EPS)
    mb = jnp.sum(bsum[...], axis=1, keepdims=True) / S
    invb = lax.rsqrt(jnp.sum(bsq[...], axis=1, keepdims=True) / S - mb * mb + EPS)
    ct = (raw[...] / S - mb * ma) * (invb * inva)
    row = lax.broadcasted_iota(jnp.int32, (256, 256), 0)
    col = lax.broadcasted_iota(jnp.int32, (256, 256), 1)
    jrow = lax.shift_right_logical(row, 5) * 512 + lax.bitwise_and(row, 31) + r * 32
    unit = jrow == col + (ft * 512 + k * 256)
    zero = jnp.zeros_like(ct)
    g = jnp.where(unit, zero, (2.0 * LAMBDA) * ct)
    g1v = (invb * g).astype(BF)
    g2v = (g * inva).astype(BF)
    g1[...] = g1v
    g2[...] = g2v
    gc = g * ct
    ua = inva * jnp.sum(gc, axis=0, keepdims=True)
    ub = invb * jnp.sum(gc, axis=1, keepdims=True)
    rowv[0:1, :] = ua
    rowv[1:2, :] = jnp.sum(g1v.astype(F32) * mb, axis=0, keepdims=True) - ma * ua
    colv[:, 0:1] = ub
    colv[:, 1:2] = jnp.sum(g2v.astype(F32) * ma, axis=1, keepdims=True) - mb * ub

    def on_diag(v):
        return jnp.sum(jnp.where(unit, v, zero), axis=0, keepdims=True)

    dtile[...] = jnp.zeros_like(dtile)
    dtile[0:1, :] = on_diag(jnp.broadcast_to(ma, ct.shape))
    dtile[1:2, :] = on_diag(jnp.broadcast_to(inva, ct.shape))
    dtile[2:3, :] = on_diag(jnp.broadcast_to(mb, ct.shape))
    dtile[3:4, :] = on_diag(jnp.broadcast_to(invb, ct.shape))
    dtile[4:5, :] = on_diag(ct)
    dtile[5:6, :] = jnp.sum(
        jnp.where(unit, (1.0 - ct) * (1.0 - ct), LAMBDA * ct * ct), axis=0, keepdims=True
    )

    def c_da(t):
        return rc(dtile, darr.at[r], I_DA, dev(lax.rem(r + t, 16), k, ft))

    def ga_block(kk, s):
        prod = lax.dot_general(
            vbt[kk, :, :, lanes(s, 128)].reshape(256, 128), g1[...],
            (((0,), (0,)), ((), ())), preferred_element_type=F32,
        )
        return prod - va[kk, s].astype(F32) * rowv[0:1, :] - rowv[1:2, :]

    def gb_block(kk, c):
        prod = lax.dot_general(
            g2[...], va[kk, pl.ds(c * 2, 2)].reshape(256, 256),
            (((1,), (1,)), ((), ())), preferred_element_type=F32,
        )
        bl = vbt[kk, :, :, lanes(c, 256)].reshape(256, 256).astype(F32)
        return (prod - bl * colv[:, 0:1] - colv[:, 1:2]).reshape(8, 32, 256)

    def c_p1p(z):
        return rc(p1p_s.at[z], p1p_r.at[z], I_P1P + z, to_xp)

    def c_p1m(z):
        return rc(p1m_s.at[z], p1m_r.at[z], I_P1M + z, to_xm)

    def c_p2p(z, h):
        return rc(p2p_s.at[z, h], p2p_r.at[z, h], I_P2P + z * 2 + h, to_xp)

    def c_p2m(z, h):
        return rc(p2m_s.at[z, h], p2m_r.at[z, h], I_P2M + z * 2 + h, to_xm)

    @pl.loop(0, 4)
    def _(z):
        s = z * 4 + x2
        p1p_s[z] = ga_block(0, s).astype(BF)
        c_p1p(z).start()
        p1m_s[z] = ga_block(1, s).astype(BF)
        c_p1m(z).start()

    darr[r] = dtile[...]

    @pl.loop(1, 16)
    def _(t):
        c_da(t).start()

    def c_gd(c):
        at = lanes(c, 512)
        return rc(gd_s.at[:, :, at], gd_r.at[:, :, at], I_GD + c, partner)

    @pl.loop(0, 4)
    def _(c):
        for e in range(2):
            gd_s[:, :, lanes(c * 2 + e, 256)] = gb_block(o, c * 2 + e).astype(BF)
        c_gd(c).start()

    @pl.loop(0, 4)
    def _(z):
        p2p_s[z, 1] = ga_block(1, z * 4 + xp).astype(BF)
        c_p2p(z, 1).start()
        p2m_s[z, 0] = ga_block(0, z * 4 + xm).astype(BF)
        c_p2m(z, 0).start()

    @pl.loop(0, 4)
    def _(z):
        aug[0, z] = ga_block(0, z * 4 + xp)
        aug[1, z] = ga_block(1, z * 4 + xm)

    @pl.loop(0, 4)
    def _(z):
        c_p1p(z).wait_recv()
        p2p_s[z, 0] = (aug[0, z] + p1p_r[z].astype(F32)).astype(BF)
        c_p2p(z, 0).start()
        c_p1m(z).wait_recv()
        p2m_s[z, 1] = (aug[1, z] + p1m_r[z].astype(F32)).astype(BF)
        c_p2m(z, 1).start()

    @pl.loop(0, 4)
    def _(c):
        c_gd(c).wait_recv()
        for e in range(2):
            at = lanes(c * 2 + e, 256)
            gb_own[:, :, at] = gb_block(k, c * 2 + e) + gd_r[:, :, at].astype(F32)

    def c_y1p(h):
        return rc(y1p_s.at[h], y1p_r.at[h], I_Y1P + h, to_yp)

    def c_y1m(h):
        return rc(y1m_s.at[h], y1m_r.at[h], I_Y1M + h, to_ym)

    def c_y2p(h, e):
        return rc(y2p_s.at[h, e], y2p_r.at[h, e], I_Y2P + h * 2 + e, to_yp)

    def c_y2m(h, e):
        return rc(y2m_s.at[h, e], y2m_r.at[h, e], I_Y2M + h * 2 + e, to_ym)

    for h in (0, 1):
        s = y2 * 2 + zhs[h]
        y1p_s[h] = gb_own[s, 0:16, :].astype(BF)
        c_y1p(h).start()
        y1m_s[h] = gb_own[s, 16:32, :].astype(BF)
        c_y1m(h).start()
    for h in (0, 1):
        y2p_s[h, 1] = gb_own[yp * 2 + zhs[h], 16:32, :].astype(BF)
        c_y2p(h, 1).start()
        y2m_s[h, 0] = gb_own[ym * 2 + zhs[h], 0:16, :].astype(BF)
        c_y2m(h, 0).start()

    rc(darr.at[0:15], darr.at[0:15], I_DA, partner).wait_recv()
    total = darr[0]
    for i in range(1, 16):
        total = total + darr[i]
    dsum[...] = total
    dboth[k] = total
    c_db = rc(dsum, dboth.at[k], I_DB, partner)
    c_db.start()

    @pl.loop(0, 4)
    def _(z):
        for h in (0, 1):
            ga_own[z, h] = ga_block(h, z * 4 + x)

    for h in (0, 1):
        c_y1p(h).wait_recv()
        y2p_s[h, 0] = (
            gb_own[yp * 2 + zhs[h], 0:16, :] + y1p_r[h].astype(F32)
        ).astype(BF)
        c_y2p(h, 0).start()
        c_y1m(h).wait_recv()
        y2m_s[h, 1] = (
            gb_own[ym * 2 + zhs[h], 16:32, :] + y1m_r[h].astype(F32)
        ).astype(BF)
        c_y2m(h, 1).start()

    c_db.wait_recv()
    both = dboth[0] + dboth[1]
    ltile[...] = both
    lz[zh] = both
    c_dz = rc(ltile, lz.at[zh], I_DZ, dev(r, k, y * 2 + zhs[1]))
    c_dz.start()

    def c_oz(q):
        return rc(oz_s.at[q - 1], oz_r.at[q - 1], I_OZ + q - 1, dev(zq[q] * 4 + x, k, ft))

    def x_sum(z):
        for h in (0, 1):
            c_p2p(z, h).wait_recv()
            c_p2m(z, h).wait_recv()
        return ga_own[z] + p2p_r[z].astype(F32) + p2m_r[z].astype(F32)

    for q in (3, 2, 1):
        oz_s[q - 1] = x_sum(zq[q]).astype(BF)
        c_oz(q).start()

    def c_a2(t, h):
        to = lax.rem(r + t, 16)
        return rc(
            a2_s.at[h, to], gfin.at[h, r], I_A2 + h, dev(to, k, y * 2 + zhs[h])
        )

    for h in (1, 0):
        for e in (0, 1):
            c_y2p(h, e).wait_recv()
            c_y2m(h, e).wait_recv()

        @pl.loop(0, 16)
        def _(t):
            at = lanes(t, 128)
            s = y * 2 + zhs[h]
            for e in (0, 1):
                a2_s[h, t, e * 16:(e + 1) * 16, :] = (
                    gb_own[s, e * 16:(e + 1) * 16, at]
                    + y2p_r[h, e, :, at].astype(F32)
                    + y2m_r[h, e, :, at].astype(F32)
                ).astype(BF)

        if h == 0:
            gfin[0, r] = a2_s[0, r]

        @pl.loop(1 - h, 16)
        def _(t):
            c_a2(t, h).start()

    c_dz.wait_recv()
    lsum = lz[0] + lz[1]
    lzsum[...] = lsum
    ly[y] = lsum

    def c_dy(j):
        return rc(lzsum, ly.at[y], I_DY + j, dev(r, k, (yp, y2, ym)[j] * 2 + zh))

    for j in range(3):
        c_dy(j).start()

    own = x_sum(zl)
    for q in (1, 2, 3):
        c_oz(q).wait_recv()
        own = own + oz_r[q - 1].astype(F32)
    od_s[...] = own
    gfa[k] = od_s[k]
    c_od = rc(od_s.at[o], gfa.at[k], I_OD, partner)
    c_od.start()

    for j in range(3):
        c_dy(j).wait_recv()
    lall = ly[0] + ly[1] + ly[2] + ly[3]
    loss_out[0, 0] = jnp.sum(lall[5:6, :]) / F

    c_od.wait_recv()
    rc(gfin.at[0, 0:15], gfin.at[0, 0:15], I_A2, partner).wait_recv()
    rc(gfin.at[1], gfin.at[1], I_A2 + 1, partner).wait_recv()
    for half in range(2):
        at = slice(half * 256, (half + 1) * 256)
        st = dboth[half]
        ma_, inva_, mb_, invb_, c_ = (st[i:i + 1, :] for i in range(5))
        an = (a_in[:, at].astype(F32) - ma_) * inva_
        bn = (b_in[:, at].astype(F32) - mb_) * invb_
        d_ = -2.0 * (1.0 - c_)
        ga_out[:, at] = (inva_ * (d_ * (bn - c_ * an) + gfa[half])).astype(BF)
        gt = (
            gfin[0, half * 8:(half + 1) * 8].reshape(256, 128).astype(F32)
            + gfin[1, half * 8:(half + 1) * 8].reshape(256, 128).astype(F32)
        )
        gb_out[:, at] = (invb_ * (d_ * (an - c_ * bn) + gt.T)).astype(BF)

    c_v0.wait_send()
    rc(vbt.at[k, ft, :, 0:1920], vbt.at[k, ft, :, 0:1920], I_W1, partner).wait_send()
    w1_all[1].wait_send()
    for q in range(4):
        for c in (c_xp, c_xm, c_xpf, c_xmf):
            c(q).wait_send()
        if q:
            c_vz(q).wait_send()
            c_oz(q).wait_send()
    for h in (0, 1):
        for c in (c_yp, c_ym, c_ypf, c_ymf, c_y1p, c_y1m):
            c(h).wait_send()
        for j in range(4):
            c_wd(j, h).wait_send()
        for e in (0, 1):
            c_y2p(h, e).wait_send()
            c_y2m(h, e).wait_send()
    for z in range(4):
        c_p1p(z).wait_send()
        c_p1m(z).wait_send()
        c_gd(z).wait_send()
        for h in (0, 1):
            c_p2p(z, h).wait_send()
            c_p2m(z, h).wait_send()
    rc(darr.at[0:15], darr.at[0:15], I_DA, partner).wait_send()
    c_db.wait_send()
    c_dz.wait_send()
    for j in range(3):
        c_dy(j).wait_send()
    c_od.wait_send()
    rc(gfin.at[0, 0:15], gfin.at[0, 0:15], I_A2, partner).wait_send()
    rc(gfin.at[1], gfin.at[1], I_A2 + 1, partner).wait_send()


def shards(view_a, view_b):
    vm = pltpu.VMEM
    block = jax.ShapeDtypeStruct(view_a.shape, BF)
    ga, gb, loss = pl.pallas_call(
        kernel,
        out_shape=(block, block, jax.ShapeDtypeStruct((1, 1), F32)),
        in_specs=[pl.BlockSpec(memory_space=vm)] * 2,
        out_specs=(
            pl.BlockSpec(memory_space=vm),
            pl.BlockSpec(memory_space=vm),
            pl.BlockSpec(memory_space=pltpu.SMEM),
        ),
        scratch_shapes=[
            vm((2, 16, 128, 256), BF),
            vm((2, 8, 32, 2048), BF),
            vm((512, 128), BF),
            vm((8, 256), F32), vm((8, 256), F32),
            vm((256, 128), F32), vm((256, 128), F32),
            vm((256, 256), F32),
            vm((256, 256), BF), vm((256, 256), BF),
            vm((8, 256), F32), vm((256, 128), F32),
            vm((8, 256), F32), vm((16, 8, 256), F32),
            vm((8, 256), F32), vm((2, 8, 256), F32),
            vm((8, 256), F32), vm((2, 8, 256), F32),
            vm((8, 256), F32), vm((4, 8, 256), F32),
            vm((4, 128, 256), BF), vm((4, 128, 256), BF),
            vm((4, 128, 256), BF), vm((4, 128, 256), BF),
            vm((2, 4, 128, 256), F32),
            vm((4, 2, 128, 256), BF), vm((4, 2, 128, 256), BF),
            vm((4, 2, 128, 256), BF), vm((4, 2, 128, 256), BF),
            vm((4, 2, 128, 256), F32),
            vm((3, 2, 128, 256), BF), vm((3, 2, 128, 256), BF),
            vm((2, 128, 256), F32), vm((2, 128, 256), F32),
            vm((8, 32, 2048), BF), vm((8, 32, 2048), BF),
            vm((8, 32, 2048), F32),
            vm((2, 16, 2048), BF), vm((2, 16, 2048), BF),
            vm((2, 16, 2048), BF), vm((2, 16, 2048), BF),
            vm((2, 2, 16, 2048), BF), vm((2, 2, 16, 2048), BF),
            vm((2, 2, 16, 2048), BF), vm((2, 2, 16, 2048), BF),
            vm((2, 16, 32, 128), BF), vm((2, 16, 32, 128), BF),
            pltpu.SemaphoreType.DMA((N_SEM,)),
            pltpu.SemaphoreType.DMA((N_SEM,)),
        ],
        compiler_params=pltpu.CompilerParams(
            collective_id=0, has_side_effects=True, vmem_limit_bytes=56 * 1024 * 1024
        ),
    )(view_a, view_b)
    return ga, gb, loss.reshape(())


def solution(mesh):
    return jax.shard_map(
        shards,
        mesh=mesh,
        in_specs=(P("dp", "feat"), P("dp", "feat")),
        out_specs=(P("dp", "feat"), P("dp", "feat"), P()),
        check_vma=False,
    )
```

```python
import jax
import jax.numpy as jnp
from jax import lax
from jax.experimental import pallas as pl
from jax.experimental.pallas import tpu as pltpu
from jax.sharding import PartitionSpec as P

F = 4096
S = 4096
EPS = 1e-05
LAMBDA = 0.0051
MESH = pl.DeviceIdType.MESH
BF = jnp.bfloat16
F32 = jnp.float32


class Slots:
    def __init__(self):
        self.used = 0

    def take(self, n):
        first = self.used
        self.used += n
        return first


SEM = Slots()
I_V1, I_W1 = (SEM.take(1) for _ in range(2))
I_GP, I_GM, I_GPF, I_GMF = (SEM.take(10) for _ in range(4))
I_ZP, I_ZM = (SEM.take(16) for _ in range(2))
I_WD = SEM.take(32)
I_SK, I_SX, I_SZ = SEM.take(1), SEM.take(3), SEM.take(3)
I_GD = SEM.take(4)
I_R1P, I_R1M = (SEM.take(10) for _ in range(2))
I_R2P, I_R2M = (SEM.take(20) for _ in range(2))
I_QP, I_QM = (SEM.take(16) for _ in range(2))
I_OZ, I_OX = (SEM.take(1) for _ in range(2))
I_LK, I_LX, I_LY, I_LZ = SEM.take(1), SEM.take(3), SEM.take(3), SEM.take(7)
N_SEM = SEM.used


def kernel(
    a_in, b_in, ga_out, gb_out, loss_out,
    at_loc, bt_loc, va, vb, stk, stx, stz, st1, st2, st3,
    asum, asq, bsum, bsq, raw, g1t, g2, cols,
    gaf, gd_s, gd_r, gbf, r1p_s, r1m_s, r1p_r, r1m_r, r2p_s, r2m_s, r2p_r, r2m_r,
    qp_s, qm_s, qp_r, qm_r, oz_s, fin_a, ox_s, fin_b,
    lt0, lt1, lt2, lt3, lk, lx, ly, lz, ssem, rsem,
):
    dp = lax.axis_index("dp")
    ft = lax.axis_index("feat")
    k = lax.rem(dp, 2)
    x = lax.rem(lax.div(dp, 2), 4)
    zl = lax.div(dp, 8)
    y, zh = lax.div(ft, 2), lax.rem(ft, 2)
    z = zh * 4 + zl
    o = 1 - k
    mb_slot = x * 4 + y
    xs = (x, lax.rem(x + 3, 4), lax.rem(x + 1, 4), lax.rem(x + 2, 4))
    ys = (y, lax.rem(y + 3, 4), lax.rem(y + 1, 4), lax.rem(y + 2, 4))
    _, xm, xp, x2 = xs
    _, ym, yp, y2 = ys

    def dev(x_, y_, z_, k_):
        return (lax.rem(z_, 4) * 8 + x_ * 2 + k_, y_ * 2 + lax.div(z_, 4))

    def zi(n):
        s = lax.rem(z + (n + 8), 8)
        return lax.div(s, 4), lax.rem(s, 4)

    def rc(src, dst, i, to):
        return pltpu.make_async_remote_copy(
            src_ref=src, dst_ref=dst, send_sem=ssem.at[i], recv_sem=rsem.at[i],
            device_id=to, device_id_type=MESH,
        )

    partner = dev(x, y, z, o)
    to_p = {"x": dev(xp, y, z, k), "y": dev(x, yp, z, k), "z": dev(x, y, lax.rem(z + 1, 8), k)}
    to_m = {"x": dev(xm, y, z, k), "y": dev(x, ym, z, k), "z": dev(x, y, lax.rem(z + 7, 8), k)}

    barrier = pltpu.get_barrier_semaphore()

    def greet(to):
        pl.semaphore_signal(barrier, inc=1, device_id=to, device_id_type=MESH)

    def plane(t):
        m = lax.rem(mb_slot + t, 16)
        return m, dev(lax.div(m, 4), lax.rem(m, 4), z, k)

    def pillar(t, k_):
        s = lax.rem(z + t, 8)
        return s, dev(x, y, s, k_)

    far_z = [(t, k_) for t in (4, 3, 5, 2, 6, 1, 7) for k_ in (k, o)] + [(0, o)]
    far_xy = (10, 14, 6, 9, 11, 2, 8, 5, 13, 7, 15, 3, 12, 4, 1)

    for t, k_ in far_z:
        greet(pillar(t, k_)[1])
    for t in far_xy:
        greet(plane(t)[1])

    for c in range(4):
        part = slice(c * 128, (c + 1) * 128)
        at_loc[2 * c:2 * c + 2] = a_in[:, part].astype(F32).T.astype(BF).reshape(2, 2, 32, 128)
    va[y, x, zh, zl, k] = at_loc[z, k]
    pl.semaphore_wait(barrier, 30)

    def c_v1(t, k_):
        s, to = pillar(t, k_)
        return rc(at_loc.at[s, k_], va.at[y, x, zh, zl, k], I_V1, to)

    def c_w1(t):
        m, to = plane(t)
        return rc(bt_loc.at[m], vb.at[zh, zl, k, y, x], I_W1, to)

    def all_pieces(i):
        return rc(bt_loc.at[0:15], bt_loc.at[0:15], i, partner)

    for t, k_ in far_z:
        c_v1(t, k_).start()
    for c in range(4):
        part = slice(c * 128, (c + 1) * 128)
        bt_loc[4 * c:4 * c + 4] = b_in[:, part].astype(F32).T.astype(BF).reshape(4, 32, 128)
    for t in far_xy:
        c_w1(t).start()
    vb[zh, zl, k, y, x] = bt_loc[mb_slot]

    af, bf = a_in[...].astype(F32), b_in[...].astype(F32)
    st1[...] = jnp.zeros_like(st1)
    for i, v in enumerate((af, af * af, bf, bf * bf, af * bf)):
        st1[i:i + 1, :] = jnp.sum(v, axis=0, keepdims=True)
    stk[k] = st1[...]
    c_sk = rc(st1, stk.at[k], I_SK, partner)
    c_sk.start()

    def ring_blocks(i):
        if i == 0:
            return "x", [va.at[y, xs[j], 0] for j in range(4)]
        if i < 5:
            return "x", [va.at[ys[i - 1], xs[j], 1] for j in range(4)]
        if i == 5:
            return "y", [va.at[ys[j], x, 1] for j in range(4)]
        return "y", [va.at[ys[j], xs[i - 6], 0] for j in range(4)]

    def c_gp(i):
        axis, b = ring_blocks(i)
        return rc(b[0], b[0], I_GP + i, to_p[axis])

    def c_gm(i):
        axis, b = ring_blocks(i)
        return rc(b[0], b[0], I_GM + i, to_m[axis])

    def c_gpf(i):
        axis, b = ring_blocks(i)
        return rc(b[1].at[0:2], b[1].at[0:2], I_GPF + i, to_p[axis])

    def c_gmf(i):
        axis, b = ring_blocks(i)
        return rc(b[2].at[2:4], b[2].at[2:4], I_GMF + i, to_m[axis])

    def ring_start(i):
        c_gp(i).start()
        c_gm(i).start()

    def ring_mid(i, then=None):
        c_gp(i).wait_recv()
        c_gpf(i).start()
        if then is not None:
            ring_start(then + 1)
        c_gm(i).wait_recv()
        c_gmf(i).start()
        if then is not None:
            ring_start(then + 2)

    def ring_end(i, then=None):
        c_gpf(i).wait_recv()
        c_gmf(i).wait_recv()
        if then is not None:
            ring_start(then + 3)

    def z_chunk(n, c):
        h_, l_ = zi(n)
        return vb.at[h_, l_, k, c]

    def c_zp(n, c):
        ref = z_chunk(-n, c)
        return rc(ref, ref, I_ZP + 4 * n + c, to_p["z"])

    def c_zm(n, c):
        ref = z_chunk(n, c)
        return rc(ref, ref, I_ZM + 4 * n + c, to_m["z"])

    def c_wd(n, c):
        ref = z_chunk(n, c)
        return rc(ref, ref, I_WD + (n % 8) * 4 + c, partner)

    def in_p(n, c):
        return n < 3 or (n == 3 and c < 2)

    def in_m(n, c):
        return n < 3 or (n == 3 and c >= 2)

    def z_step(n):
        for c in range(4):
            if in_p(n, c):
                c_zp(n, c).wait_recv()
                if in_p(n + 1, c):
                    c_zp(n + 1, c).start()
                c_wd(-(n + 1), c).start()
            if in_m(n, c):
                c_zm(n, c).wait_recv()
                if in_m(n + 1, c):
                    c_zm(n + 1, c).start()
                c_wd(n + 1, c).start()

    all_pieces(I_V1).wait_recv()
    ring_start(0)
    ring_start(5)
    ring_start(1)
    ring_start(6)
    all_pieces(I_W1).wait_recv()
    for c in range(4):
        c_zp(0, c).start()
        c_zm(0, c).start()
    for c in range(4):
        c_wd(0, c).start()

    c_sk.wait_recv()
    sk = stk[0] + stk[1]
    st2[...] = sk
    stx[x] = sk

    def c_sx(j):
        return rc(st2, stx.at[x], I_SX + j, dev((xm, xp, x2)[j], y, z, k))

    for j in range(3):
        c_sx(j).start()

    ring_mid(0, then=6)
    ring_mid(5, then=1)
    z_step(0)
    ring_end(0, then=6)
    ring_end(5, then=1)

    for j in range(3):
        c_sx(j).wait_recv()
    sx = (stx[0] + stx[1]) + (stx[2] + stx[3])
    st3[...] = sx
    stz[zl] = sx

    def c_sz(j):
        l_ = lax.rem(zl + (j + 1), 4)
        return rc(st3, stz.at[zl], I_SZ + j, dev(x, y, zh * 4 + l_, k))

    for j in range(3):
        c_sz(j).start()

    ring_mid(1)
    ring_mid(6)
    z_step(1)
    ring_mid(2)
    ring_mid(7)
    ring_mid(3)
    ring_mid(8)
    z_step(2)
    ring_mid(4)
    ring_mid(9)
    z_step(3)
    for i in (1, 6, 2, 7, 3, 8, 4, 9):
        ring_end(i)
    for n in range(8):
        for c in range(4):
            c_wd(n, c).wait_recv()

    for ref in (asum, asq, bsum, bsq, raw):
        ref[...] = jnp.zeros_like(ref)

    def va_at(x_, l_, kk):
        return va[:, x_, :, l_, kk].reshape(256, 128)

    def vb_at(x_, l_, kk):
        return vb[:, l_, kk, :, x_].reshape(256, 128)

    @pl.loop(0, 16)
    def _(t):
        x_, l_ = lax.div(t, 4), lax.rem(t, 4)
        a0, a1 = va_at(x_, l_, 0), va_at(x_, l_, 1)
        b0, b1 = vb_at(x_, l_, 0), vb_at(x_, l_, 1)
        raw[...] += lax.dot_general(
            jnp.concatenate([b0, b1], axis=1), jnp.concatenate([a0, a1], axis=1),
            (((1,), (1,)), ((), ())), preferred_element_type=F32,
        )
        for p0, p1, s_, q_ in ((a0, a1, asum, asq), (b0, b1, bsum, bsq)):
            f0, f1 = p0.astype(F32), p1.astype(F32)
            s_[...] += f0 + f1
            q_[...] += f0 * f0 + f1 * f1

    row = lax.broadcasted_iota(jnp.int32, (256, 256), 0)
    col = lax.broadcasted_iota(jnp.int32, (256, 256), 1)
    zero = jnp.zeros((256, 256), F32)
    eye = row == col

    def to_row(v):
        return jnp.sum(jnp.where(eye, v, zero), axis=0, keepdims=True)

    def to_col(v):
        return jnp.sum(jnp.where(eye, v, zero), axis=1, keepdims=True)

    ma = jnp.sum(asum[...], axis=1, keepdims=True) / S
    inva = lax.rsqrt(jnp.sum(asq[...], axis=1, keepdims=True) / S - ma * ma + EPS)
    mb = jnp.sum(bsum[...], axis=1, keepdims=True) / S
    invb = lax.rsqrt(jnp.sum(bsq[...], axis=1, keepdims=True) / S - mb * mb + EPS)
    ma_r, inva_r = to_row(ma), to_row(inva)
    ct = (raw[...] / S - mb * ma_r) * (invb * inva_r)

    def bits(v, shift, mask):
        return lax.bitwise_and(lax.shift_right_logical(v, shift), mask)

    j_id = (bits(row, 5, 3) * 2 + bits(row, 7, 1)) * 512 + mb_slot * 32 + bits(row, 0, 31)
    i_id = bits(col, 5, 7) * 512 + (z * 2 + k) * 32 + bits(col, 0, 31)
    unit = j_id == i_id
    g = jnp.where(unit, zero, (2.0 * LAMBDA) * ct)
    g1 = (invb * g).astype(BF).astype(F32)
    g1t[...] = g1.T.astype(BF)
    g2v = (g * inva_r).astype(BF)
    g2[...] = g2v
    gc = g * ct
    ua = inva * to_col(jnp.sum(gc, axis=0, keepdims=True))
    ub = invb * jnp.sum(gc, axis=1, keepdims=True)
    cols[:, 0:1] = ua
    cols[:, 1:2] = to_col(jnp.sum(g1 * mb, axis=0, keepdims=True)) - ma * ua
    cols[:, 2:3] = ub
    cols[:, 3:4] = jnp.sum(g2v.astype(F32) * ma_r, axis=1, keepdims=True) - mb * ub
    lv = jnp.sum(
        jnp.where(unit, (1.0 - ct) * (1.0 - ct), LAMBDA * ct * ct), axis=0, keepdims=True
    )
    l0 = jnp.broadcast_to(lv[:, 0:128] + lv[:, 128:256], (8, 128))
    lt0[...] = l0
    lk[k] = l0
    c_lk = rc(lt0, lk.at[k], I_LK, partner)
    c_lk.start()

    def near(j):
        return lax.rem(zl + (0, 1, 3, 2)[j], 4)

    def gb_pair(x_, l_, kk):
        a0, a1 = va_at(x_, l_, kk), va_at(x_ + 1, l_, kk)
        prod = jnp.dot(g2[...], jnp.concatenate([a0, a1], axis=1), preferred_element_type=F32)
        return [
            prod[:, e * 128:(e + 1) * 128]
            - vb_at(x_ + e, l_, kk).astype(F32) * cols[:, 2:3] - cols[:, 3:4]
            for e in (0, 1)
        ]

    def c_gd(j):
        return rc(gd_s.at[j], gd_r.at[j], I_GD + j, partner)

    for j in range(4):
        for x_ in (0, 2):
            for e, v in enumerate(gb_pair(x_, near(j), o)):
                gd_s[j, x_ + e] = v.astype(BF)
        c_gd(j).start()

    def ga_strip(x_):
        @pl.loop(0, 4)
        def _(l_):
            b01 = jnp.concatenate([vb_at(x_, l_, 0), vb_at(x_, l_, 1)], axis=1)
            prod = jnp.dot(g1t[...], b01, preferred_element_type=F32)
            for e in (0, 1):
                gaf[:, x_, :, l_, e] = (
                    prod[:, e * 128:(e + 1) * 128]
                    - va_at(x_, l_, e).astype(F32) * cols[:, 0:1] - cols[:, 1:2]
                ).reshape(4, 2, 32, 128)

    def axis_of(i):
        return "x" if i < 5 else "y"

    def part(i, j):
        if i == 0:
            return gaf[y, xs[j], 0]
        if i < 5:
            return gaf[ys[i - 1], xs[j], 1]
        if i == 5:
            return gaf[ys[j], x, 1]
        return gaf[ys[j], xs[i - 6], 0]

    def c_r1p(i):
        return rc(r1p_s.at[i], r1p_r.at[i], I_R1P + i, to_p[axis_of(i)])

    def c_r1m(i):
        return rc(r1m_s.at[i], r1m_r.at[i], I_R1M + i, to_m[axis_of(i)])

    def c_r2p(i, h):
        at = slice(2 * h, 2 * h + 2)
        return rc(r2p_s.at[i, at], r2p_r.at[i, at], I_R2P + 2 * i + h, to_p[axis_of(i)])

    def c_r2m(i, h):
        at = slice(2 * h, 2 * h + 2)
        return rc(r2m_s.at[i, at], r2m_r.at[i, at], I_R2M + 2 * i + h, to_m[axis_of(i)])

    def red_first(i):
        far = part(i, 3)
        r1p_s[i] = far[0:2].astype(BF)
        c_r1p(i).start()
        r1m_s[i] = far[2:4].astype(BF)
        c_r1m(i).start()

    def red_free(i):
        r2p_s[i, 2:4] = part(i, 2)[2:4].astype(BF)
        c_r2p(i, 1).start()
        r2m_s[i, 0:2] = part(i, 1)[0:2].astype(BF)
        c_r2m(i, 0).start()

    def red_mid(i):
        c_r1p(i).wait_recv()
        r2p_s[i, 0:2] = (part(i, 2)[0:2] + r1p_r[i].astype(F32)).astype(BF)
        c_r2p(i, 0).start()
        c_r1m(i).wait_recv()
        r2m_s[i, 2:4] = (part(i, 1)[2:4] + r1m_r[i].astype(F32)).astype(BF)
        c_r2m(i, 1).start()

    def red_end(i):
        for h in (0, 1):
            c_r2p(i, h).wait_recv()
            c_r2m(i, h).wait_recv()
        return part(i, 0) + r2p_r[i].astype(F32) + r2m_r[i].astype(F32)

    def gb_own(j):
        c_gd(j).wait_recv()
        for x_ in (0, 2):
            for e, v in enumerate(gb_pair(x_, near(j), k)):
                v = v + gd_r[j, x_ + e].astype(F32)
                gbf[:, near(j), :, x_ + e] = v.reshape(2, 4, 32, 128)

    def z_part(n, c):
        h_, l_ = zi(n)
        return gbf[h_, l_, c]

    def c_qp(n, c):
        return rc(qp_s.at[n, c], qp_r.at[n, c], I_QP + 4 * n + c, to_p["z"])

    def c_qm(n, c):
        return rc(qm_s.at[n, c], qm_r.at[n, c], I_QM + 4 * n + c, to_m["z"])

    def q_send(n, first):
        for c in range(4):
            if in_p(3 - n, c) and in_p(4 - n, c) != first:
                v = z_part(4 - n, c)
                if not first:
                    c_qp(n - 1, c).wait_recv()
                    v = v + qp_r[n - 1, c].astype(F32)
                qp_s[n, c] = v.astype(BF)
                c_qp(n, c).start()
            if in_m(3 - n, c) and in_m(4 - n, c) != first:
                v = z_part(n - 4, c)
                if not first:
                    c_qm(n - 1, c).wait_recv()
                    v = v + qm_r[n - 1, c].astype(F32)
                qm_s[n, c] = v.astype(BF)
                c_qm(n, c).start()

    ga_strip(x2)
    red_first(9)
    for i in (4, 3, 2, 1):
        red_first(i)
    gb_own(0)
    q_send(0, True)
    gb_own(1)
    gb_own(2)
    q_send(1, True)
    gb_own(3)
    ga_strip(xp)
    red_first(8)
    ga_strip(xm)
    red_first(7)
    for i in (9, 4, 8, 7, 3, 2, 1):
        red_free(i)
    ga_strip(x)
    red_first(6)
    red_free(6)
    red_mid(9)
    red_mid(4)
    q_send(1, False)
    red_mid(8)
    red_mid(3)
    red_mid(7)
    red_mid(2)

    def c_lx(j):
        return rc(lt1, lx.at[x], I_LX + j, dev((xm, xp, x2)[j], y, z, k))

    def c_ly(j):
        return rc(lt2, ly.at[y], I_LY + j, dev(x, (ym, yp, y2)[j], z, k))

    def c_lz(j):
        return rc(lt3, lz.at[z], I_LZ + j, pillar(j + 1, k)[1])

    c_lk.wait_recv()
    l1 = lk[0] + lk[1]
    lt1[...] = l1
    lx[x] = l1
    for j in range(3):
        c_lx(j).start()

    gaf[y, x2, 0] = red_end(9)
    red_first(0)
    gaf[y2, x, 1] = red_end(4)
    red_first(5)
    red_mid(6)
    red_mid(1)
    q_send(2, False)
    gaf[y, xp, 0] = red_end(8)
    gaf[y, xm, 0] = red_end(7)
    red_free(0)
    gaf[yp, x, 1] = red_end(3)
    gaf[ym, x, 1] = red_end(2)
    red_free(5)
    red_mid(0)
    red_mid(5)
    for j in range(3):
        c_lx(j).wait_recv()
    l2 = (lx[0] + lx[1]) + (lx[2] + lx[3])
    lt2[...] = l2
    ly[y] = l2
    for j in range(3):
        c_ly(j).start()
    q_send(3, False)
    gaf[y, x, 0] = red_end(6)
    gaf[y, x, 1] = red_end(1)

    def c_ox(t):
        m, to = plane(t)
        return rc(ox_s.at[m], fin_b.at[mb_slot], I_OX, to)

    for c in range(4):
        c_qp(3, c).wait_recv()
        c_qm(3, c).wait_recv()
        v = z_part(0, c) + qp_r[3, c].astype(F32) + qm_r[3, c].astype(F32)
        for x_ in range(4):
            ox_s[x_ * 4 + c] = v[x_].astype(BF)
    for t in far_xy:
        c_ox(t).start()
    fin_b[mb_slot] = ox_s[mb_slot]
    for j in range(3):
        c_ly(j).wait_recv()
    l3 = (ly[0] + ly[1]) + (ly[2] + ly[3])
    lt3[...] = l3
    lz[z] = l3
    for j in range(7):
        c_lz(j).start()

    def c_oz(t, k_):
        s, to = pillar(t, k_)
        return rc(oz_s.at[s, k_], fin_a.at[z, k], I_OZ, to)

    oz_s[0:4] = red_end(0).astype(BF)
    oz_s[4:8] = red_end(5).astype(BF)
    for t, k_ in far_z:
        c_oz(t, k_).start()
    fin_a[z, k] = oz_s[z, k]

    for j in range(3):
        c_sz(j).wait_recv()
    st = ((stz[0] + stz[1]) + (stz[2] + stz[3])) / S
    ma_, mb_ = st[0:1], st[2:3]
    inva_ = lax.rsqrt(st[1:2] - ma_ * ma_ + EPS)
    invb_ = lax.rsqrt(st[3:4] - mb_ * mb_ + EPS)
    c_ = (st[4:5] - ma_ * mb_) * (inva_ * invb_)
    d_ = -2.0 * (1.0 - c_)

    for j in range(7):
        c_lz(j).wait_recv()
    lall = lz[0]
    for i in range(1, 8):
        lall = lall + lz[i]
    loss_out[0, 0] = jnp.sum(lall[0:1, :]) / F

    all_pieces(I_OX).wait_recv()
    for c in range(4):
        at = slice(c * 128, (c + 1) * 128)
        an = (a_in[:, at].astype(F32) - ma_[:, at]) * inva_[:, at]
        bn = (b_in[:, at].astype(F32) - mb_[:, at]) * invb_[:, at]
        gt = fin_b[4 * c:4 * c + 4].reshape(128, 128).astype(F32).T
        gb_out[:, at] = (invb_[:, at] * (d_[:, at] * (an - c_[:, at] * bn) + gt)).astype(BF)

    all_pieces(I_OZ).wait_recv()
    for c in range(4):
        at = slice(c * 128, (c + 1) * 128)
        an = (a_in[:, at].astype(F32) - ma_[:, at]) * inva_[:, at]
        bn = (b_in[:, at].astype(F32) - mb_[:, at]) * invb_[:, at]
        gt = fin_a[2 * c:2 * c + 2].reshape(128, 128).astype(F32).T
        ga_out[:, at] = (inva_[:, at] * (d_[:, at] * (bn - c_[:, at] * an) + gt)).astype(BF)

    for c in (c_sk, c_lk):
        c.wait_send()
    for i in (I_V1, I_W1, I_OX, I_OZ):
        all_pieces(i).wait_send()
    for j in range(3):
        for c in (c_sx, c_sz, c_lx, c_ly):
            c(j).wait_send()
    for j in range(7):
        c_lz(j).wait_send()
    for i in range(4):
        c_gd(i).wait_send()
    for i in range(10):
        for c in (c_gp, c_gm, c_gpf, c_gmf, c_r1p, c_r1m):
            c(i).wait_send()
        for h in (0, 1):
            c_r2p(i, h).wait_send()
            c_r2m(i, h).wait_send()
    for n in range(8):
        for c in range(4):
            c_wd(n, c).wait_send()
    for n in range(4):
        for c in range(4):
            if in_p(n, c):
                c_zp(n, c).wait_send()
            if in_m(n, c):
                c_zm(n, c).wait_send()
            if in_p(3 - n, c):
                c_qp(n, c).wait_send()
            if in_m(3 - n, c):
                c_qm(n, c).wait_send()


def shards(view_a, view_b):
    vm = pltpu.VMEM
    block = jax.ShapeDtypeStruct(view_a.shape, BF)
    ga, gb, loss = pl.pallas_call(
        kernel,
        out_shape=(block, block, jax.ShapeDtypeStruct((1, 1), F32)),
        in_specs=[pl.BlockSpec(memory_space=vm)] * 2,
        out_specs=(
            pl.BlockSpec(memory_space=vm),
            pl.BlockSpec(memory_space=vm),
            pl.BlockSpec(memory_space=pltpu.SMEM),
        ),
        scratch_shapes=[
            vm((8, 2, 32, 128), BF), vm((16, 32, 128), BF),
            vm((4, 4, 2, 4, 2, 32, 128), BF),
            vm((2, 4, 2, 4, 4, 32, 128), BF),
            vm((2, 8, 512), F32), vm((4, 8, 512), F32), vm((4, 8, 512), F32),
            vm((8, 512), F32), vm((8, 512), F32), vm((8, 512), F32),
            *[vm((256, 128), F32)] * 4,
            vm((256, 256), F32), vm((256, 256), BF), vm((256, 256), BF),
            vm((256, 128), F32),
            vm((4, 4, 2, 4, 2, 32, 128), F32),
            vm((4, 4, 256, 128), BF), vm((4, 4, 256, 128), BF),
            vm((2, 4, 4, 4, 32, 128), F32),
            *[vm((10, 2, 2, 32, 128), BF)] * 4,
            *[vm((10, 4, 2, 32, 128), BF)] * 4,
            *[vm((4, 4, 4, 32, 128), BF)] * 4,
            vm((8, 2, 32, 128), BF), vm((8, 2, 32, 128), BF),
            vm((16, 32, 128), BF), vm((16, 32, 128), BF),
            *[vm((8, 128), F32)] * 4,
            vm((2, 8, 128), F32), vm((4, 8, 128), F32), vm((4, 8, 128), F32), vm((8, 8, 128), F32),
            pltpu.SemaphoreType.DMA((N_SEM,)),
            pltpu.SemaphoreType.DMA((N_SEM,)),
        ],
        compiler_params=pltpu.CompilerParams(
            collective_id=0, has_side_effects=True, vmem_limit_bytes=56 * 1024 * 1024
        ),
    )(view_a, view_b)
    return ga, gb, loss.reshape(())


def solution(mesh):
    return jax.shard_map(
        shards,
        mesh=mesh,
        in_specs=(P("dp", "feat"), P("dp", "feat")),
        out_specs=(P("dp", "feat"), P("dp", "feat"), P()),
        check_vma=False,
    )
```

```python
import jax
import jax.numpy as jnp
from jax import lax
from jax.experimental import pallas as pl
from jax.experimental.pallas import tpu as pltpu
from jax.sharding import PartitionSpec as P

F = 4096
S = 4096
EPS = 1e-05
LAMBDA = 0.0051
MESH = pl.DeviceIdType.MESH
BF = jnp.bfloat16
F32 = jnp.float32


class Slots:
    def __init__(self):
        self.used = 0

    def take(self, n):
        first = self.used
        self.used += n
        return first


SEM = Slots()
I_V1, I_W1, I_SK, I_SX, I_SZ, I_OZ, I_OX, I_LK, I_LX, I_LY, I_LZ = (SEM.take(1) for _ in range(11))
I_GP, I_GM, I_GF = (SEM.take(10) for _ in range(3))
I_ZP, I_ZM = (SEM.take(14) for _ in range(2))
I_WD = SEM.take(8)
I_GD = SEM.take(4)
I_R1P, I_R1M, I_R2 = (SEM.take(10) for _ in range(3))
I_QP, I_QM = (SEM.take(14) for _ in range(2))
N_RECV = SEM.used
OUT = Slots()
(O_V1, O_W1, O_SK, O_SX, O_SZ, O_OZ, O_OX, O_LK, O_LX, O_LY, O_LZ,
 O_GP, O_GM, O_GPF, O_GMF, O_WD, O_GD, O_R1P, O_R1M, O_R2P, O_R2M) = (OUT.take(1) for _ in range(21))
O_ZP, O_ZM, O_QP, O_QM = (OUT.take(2) for _ in range(4))
N_SEND = OUT.used


def kernel(
    a_hbm, b_hbm, ga_out, gb_out, loss_out,
    a_in, b_in, at_loc, bt_loc, va, vb, stk, stx, stz, st1, st2, st3,
    asum, asq, bsum, bsq, raw, g1t, g2, cols,
    gaf, gd_s, gd_r, gbf, r1p_s, r1m_s, r1p_r, r1m_r, r2p_s, r2m_s, r2p_r, r2m_r,
    qp_s, qm_s, qp_r, qm_r, oz_s, fin_a, ox_s, fin_b,
    lt0, lt1, lt2, lt3, lk, lx, ly, lz, ssem, rsem, isem,
):
    dp = lax.axis_index("dp")
    ft = lax.axis_index("feat")
    k = lax.rem(dp, 2)
    x = lax.rem(lax.div(dp, 2), 4)
    zl = lax.div(dp, 8)
    y, zh = lax.div(ft, 2), lax.rem(ft, 2)
    z = zh * 4 + zl
    o = 1 - k
    mb_slot = x * 4 + y
    xs = (x, lax.rem(x + 3, 4), lax.rem(x + 1, 4), lax.rem(x + 2, 4))
    ys = (y, lax.rem(y + 3, 4), lax.rem(y + 1, 4), lax.rem(y + 2, 4))
    _, xm, xp, x2 = xs
    _, ym, yp, y2 = ys

    def dev(x_, y_, z_, k_):
        return (lax.rem(z_, 4) * 8 + x_ * 2 + k_, y_ * 2 + lax.div(z_, 4))

    def zi(n):
        s = lax.rem(z + (n + 8), 8)
        return lax.div(s, 4), lax.rem(s, 4)

    def rc(src, dst, i, e, to):
        return pltpu.make_async_remote_copy(
            src_ref=src, dst_ref=dst, send_sem=ssem.at[e], recv_sem=rsem.at[i],
            device_id=to, device_id_type=MESH,
        )

    def landed(ref, i):
        rc(ref, ref, i, 0, partner).wait_recv()

    def left(ref, e):
        rc(ref, ref, 0, e, partner).wait_send()

    partner = dev(x, y, z, o)
    to_p = {"x": dev(xp, y, z, k), "y": dev(x, yp, z, k), "z": dev(x, y, lax.rem(z + 1, 8), k)}
    to_m = {"x": dev(xm, y, z, k), "y": dev(x, ym, z, k), "z": dev(x, y, lax.rem(z + 7, 8), k)}

    barrier = pltpu.get_barrier_semaphore()

    def greet(to):
        pl.semaphore_signal(barrier, inc=1, device_id=to, device_id_type=MESH)

    def plane(t):
        m = lax.rem(mb_slot + t, 16)
        return m, dev(lax.div(m, 4), lax.rem(m, 4), z, k)

    def pillar(t, k_):
        s = lax.rem(z + t, 8)
        return s, dev(x, y, s, k_)

    load_a = pltpu.make_async_copy(a_hbm, a_in, isem.at[0])
    load_b = pltpu.make_async_copy(b_hbm, b_in, isem.at[1])
    load_a.start()
    load_b.start()

    far_z = [(t, k_) for t in (4, 3, 5, 2, 6, 1, 7) for k_ in (k, o)] + [(0, o)]
    far_xy = (10, 14, 6, 9, 11, 2, 8, 5, 13, 7, 15, 3, 12, 4, 1)

    for t, k_ in far_z:
        greet(pillar(t, k_)[1])
    for t in far_xy:
        greet(plane(t)[1])

    load_a.wait()
    for c in range(4):
        part = slice(c * 128, (c + 1) * 128)
        at_loc[2 * c:2 * c + 2] = a_in[:, part].astype(F32).T.astype(BF).reshape(2, 2, 32, 128)
    va[y, x, zh, zl, k] = at_loc[z, k]
    pl.semaphore_wait(barrier, 30)

    def c_v1(t, k_):
        s, to = pillar(t, k_)
        return rc(at_loc.at[s, k_], va.at[y, x, zh, zl, k], I_V1, O_V1, to)

    def c_w1(t):
        m, to = plane(t)
        return rc(bt_loc.at[m], vb.at[zh, zl, k, y, x], I_W1, O_W1, to)

    for t, k_ in far_z:
        c_v1(t, k_).start()
    load_b.wait()
    for c in range(4):
        part = slice(c * 128, (c + 1) * 128)
        bt_loc[4 * c:4 * c + 4] = b_in[:, part].astype(F32).T.astype(BF).reshape(4, 32, 128)
    for t in far_xy:
        c_w1(t).start()
    vb[zh, zl, k, y, x] = bt_loc[mb_slot]

    af, bf = a_in[...].astype(F32), b_in[...].astype(F32)
    st1[...] = jnp.zeros_like(st1)
    for i, v in enumerate((af, af * af, bf, bf * bf, af * bf)):
        st1[i:i + 1, :] = jnp.sum(v, axis=0, keepdims=True)
    stk[k] = st1[...]
    c_sk = rc(st1, stk.at[k], I_SK, O_SK, partner)
    c_sk.start()

    def ring_blocks(i):
        if i == 0:
            return "x", [va.at[y, xs[j], 0] for j in range(4)]
        if i < 5:
            return "x", [va.at[ys[i - 1], xs[j], 1] for j in range(4)]
        if i == 5:
            return "y", [va.at[ys[j], x, 1] for j in range(4)]
        return "y", [va.at[ys[j], xs[i - 6], 0] for j in range(4)]

    def c_gp(i):
        axis, b = ring_blocks(i)
        return rc(b[0], b[0], I_GP + i, O_GP, to_p[axis])

    def c_gm(i):
        axis, b = ring_blocks(i)
        return rc(b[0], b[0], I_GM + i, O_GM, to_m[axis])

    def c_gpf(i):
        axis, b = ring_blocks(i)
        return rc(b[1].at[0:2], b[1].at[0:2], I_GF + i, O_GPF, to_p[axis])

    def c_gmf(i):
        axis, b = ring_blocks(i)
        return rc(b[2].at[2:4], b[2].at[2:4], I_GF + i, O_GMF, to_m[axis])

    def ring_start(i):
        c_gp(i).start()
        c_gm(i).start()

    def ring_mid(i, then=None):
        c_gp(i).wait_recv()
        c_gpf(i).start()
        if then is not None:
            ring_start(then + 1)
        c_gm(i).wait_recv()
        c_gmf(i).start()
        if then is not None:
            ring_start(then + 2)

    def ring_end(i, then=None):
        landed(ring_blocks(i)[1][3], I_GF + i)
        if then is not None:
            ring_start(then + 3)

    def z_chunk(n, c):
        h_, l_ = zi(n)
        return vb.at[h_, l_, k, c]

    def c_zp(n, c):
        ref = z_chunk(-n, c)
        return rc(ref, ref, I_ZP + 4 * n + c, O_ZP + n // 3, to_p["z"])

    def c_zm(n, c):
        ref = z_chunk(n, c)
        return rc(ref, ref, I_ZM + 4 * n + c - 2 * (n // 3), O_ZM + n // 3, to_m["z"])

    def c_wd(n, c):
        ref = z_chunk(n, c)
        return rc(ref, ref, I_WD + n % 8, O_WD, partner)

    def in_p(n, c):
        return n < 3 or (n == 3 and c < 2)

    def in_m(n, c):
        return n < 3 or (n == 3 and c >= 2)

    def z_step(n):
        for c in range(4):
            if in_p(n, c):
                c_zp(n, c).wait_recv()
                if in_p(n + 1, c):
                    c_zp(n + 1, c).start()
                c_wd(-(n + 1), c).start()
            if in_m(n, c):
                c_zm(n, c).wait_recv()
                if in_m(n + 1, c):
                    c_zm(n + 1, c).start()
                c_wd(n + 1, c).start()

    landed(bt_loc.at[0:15], I_V1)
    ring_start(0)
    ring_start(5)
    ring_start(1)
    ring_start(6)
    landed(bt_loc.at[0:15], I_W1)
    for c in range(4):
        c_zp(0, c).start()
        c_zm(0, c).start()
    for c in range(4):
        c_wd(0, c).start()

    c_sk.wait_recv()
    sk = stk[0] + stk[1]
    st2[...] = sk
    stx[x] = sk

    def c_sx(j):
        return rc(st2, stx.at[x], I_SX, O_SX, dev((xm, xp, x2)[j], y, z, k))

    for j in range(3):
        c_sx(j).start()

    ring_mid(0, then=6)
    ring_mid(5, then=1)
    z_step(0)
    ring_end(0, then=6)
    ring_end(5, then=1)

    landed(stx.at[0:3], I_SX)
    sx = (stx[0] + stx[1]) + (stx[2] + stx[3])
    st3[...] = sx
    stz[zl] = sx

    def c_sz(j):
        l_ = lax.rem(zl + (j + 1), 4)
        return rc(st3, stz.at[zl], I_SZ, O_SZ, dev(x, y, zh * 4 + l_, k))

    for j in range(3):
        c_sz(j).start()

    for ref in (asum, asq, bsum, bsq, raw):
        ref[...] = jnp.zeros_like(ref)

    def va_at(x_, l_, kk):
        return va[:, x_, :, l_, kk].reshape(256, 128)

    def vb_at(x_, l_, kk):
        return vb[:, l_, kk, :, x_].reshape(256, 128)

    def near(j):
        return lax.rem(zl + (0, 1, 3, 2)[j], 4)

    def corr(j):
        l_ = near(j)

        pairs = [(x_, kk) for x_ in range(4) for kk in (0, 1)]
        a_, b_ = ([f(x_, l_, kk) for x_, kk in pairs] for f in (va_at, vb_at))
        raw[...] += lax.dot_general(
            jnp.concatenate(b_, axis=1), jnp.concatenate(a_, axis=1),
            (((1,), (1,)), ((), ())), preferred_element_type=F32,
        )
        for f, s_, q_ in ((va_at, asum, asq), (vb_at, bsum, bsq)):
            for h in range(4):
                at = slice(h * 64, h * 64 + 64)
                v = [f(x_, l_, kk)[at].astype(F32) for x_, kk in pairs]
                s_[at, :] += sum(v[1:], v[0])
                q_[at, :] += sum((u * u for u in v[1:]), v[0] * v[0])

    def from_core(n):
        h_, l_ = zi(n)
        landed(vb.at[h_, l_, o], I_WD + n % 8)

    ring_mid(1)
    ring_mid(6)
    z_step(1)
    ring_mid(2)
    ring_mid(7)
    ring_mid(3)
    ring_mid(8)
    z_step(2)
    ring_mid(4)
    ring_mid(9)
    for i in (1, 6, 2, 7, 3, 8, 4, 9):
        ring_end(i)
    z_step(3)
    from_core(2)
    from_core(-2)
    corr(3)
    from_core(1)
    from_core(-3)
    corr(1)
    from_core(-1)
    from_core(3)
    corr(2)
    from_core(0)
    from_core(4)
    corr(0)
    row = lax.broadcasted_iota(jnp.int32, (256, 256), 0)
    col = lax.broadcasted_iota(jnp.int32, (256, 256), 1)
    zero = jnp.zeros((256, 256), F32)
    eye = row == col

    def to_row(v):
        return jnp.sum(jnp.where(eye, v, zero), axis=0, keepdims=True)

    def to_col(v):
        return jnp.sum(jnp.where(eye, v, zero), axis=1, keepdims=True)

    ma = jnp.sum(asum[...], axis=1, keepdims=True) / S
    inva = lax.rsqrt(jnp.sum(asq[...], axis=1, keepdims=True) / S - ma * ma + EPS)
    mb = jnp.sum(bsum[...], axis=1, keepdims=True) / S
    invb = lax.rsqrt(jnp.sum(bsq[...], axis=1, keepdims=True) / S - mb * mb + EPS)
    ma_r, inva_r = to_row(ma), to_row(inva)
    ct = (raw[...] / S - mb * ma_r) * (invb * inva_r)

    def bits(v, shift, mask):
        return lax.bitwise_and(lax.shift_right_logical(v, shift), mask)

    j_id = (bits(row, 5, 3) * 2 + bits(row, 7, 1)) * 512 + mb_slot * 32 + bits(row, 0, 31)
    i_id = bits(col, 5, 7) * 512 + (z * 2 + k) * 32 + bits(col, 0, 31)
    unit = j_id == i_id
    g = jnp.where(unit, zero, (2.0 * LAMBDA) * ct)
    g1 = (invb * g).astype(BF).astype(F32)
    g1t[...] = g1.T.astype(BF)
    g2v = (g * inva_r).astype(BF)
    g2[...] = g2v
    gc = g * ct
    ua = inva * to_col(jnp.sum(gc, axis=0, keepdims=True))
    ub = invb * jnp.sum(gc, axis=1, keepdims=True)
    cols[:, 0:1] = ua
    cols[:, 1:2] = to_col(jnp.sum(g1 * mb, axis=0, keepdims=True)) - ma * ua
    cols[:, 2:3] = ub
    cols[:, 3:4] = jnp.sum(g2v.astype(F32) * ma_r, axis=1, keepdims=True) - mb * ub
    lv = jnp.sum(
        jnp.where(unit, (1.0 - ct) * (1.0 - ct), LAMBDA * ct * ct), axis=0, keepdims=True
    )
    l0 = jnp.broadcast_to(lv[:, 0:128] + lv[:, 128:256], (8, 128))
    lt0[...] = l0
    lk[k] = l0
    c_lk = rc(lt0, lk.at[k], I_LK, O_LK, partner)
    c_lk.start()

    def gb_pair(x_, l_, kk):
        a0, a1 = va_at(x_, l_, kk), va_at(x_ + 1, l_, kk)
        prod = jnp.dot(g2[...], jnp.concatenate([a0, a1], axis=1), preferred_element_type=F32)
        return [
            prod[:, e * 128:(e + 1) * 128]
            - vb_at(x_ + e, l_, kk).astype(F32) * cols[:, 2:3] - cols[:, 3:4]
            for e in (0, 1)
        ]

    def c_gd(j):
        return rc(gd_s.at[j], gd_r.at[j], I_GD + j, O_GD, partner)

    for j in range(4):
        for x_ in (0, 2):
            for e, v in enumerate(gb_pair(x_, near(j), o)):
                gd_s[j, x_ + e] = v.astype(BF)
        c_gd(j).start()

    def ga_strip(x_):
        @pl.loop(0, 4)
        def _(l_):
            b01 = jnp.concatenate([vb_at(x_, l_, 0), vb_at(x_, l_, 1)], axis=1)
            prod = jnp.dot(g1t[...], b01, preferred_element_type=F32)
            for e in (0, 1):
                gaf[:, x_, :, l_, e] = (
                    prod[:, e * 128:(e + 1) * 128]
                    - va_at(x_, l_, e).astype(F32) * cols[:, 0:1] - cols[:, 1:2]
                ).reshape(4, 2, 32, 128)

    def axis_of(i):
        return "x" if i < 5 else "y"

    def part(i, j):
        if i == 0:
            return gaf[y, xs[j], 0]
        if i < 5:
            return gaf[ys[i - 1], xs[j], 1]
        if i == 5:
            return gaf[ys[j], x, 1]
        return gaf[ys[j], xs[i - 6], 0]

    def c_r1p(i):
        return rc(r1p_s.at[i], r1p_r.at[i], I_R1P + i, O_R1P, to_p[axis_of(i)])

    def c_r1m(i):
        return rc(r1m_s.at[i], r1m_r.at[i], I_R1M + i, O_R1M, to_m[axis_of(i)])

    def c_r2p(i, h):
        at = slice(2 * h, 2 * h + 2)
        return rc(r2p_s.at[i, at], r2p_r.at[i, at], I_R2 + i, O_R2P, to_p[axis_of(i)])

    def c_r2m(i, h):
        at = slice(2 * h, 2 * h + 2)
        return rc(r2m_s.at[i, at], r2m_r.at[i, at], I_R2 + i, O_R2M, to_m[axis_of(i)])

    def red_first(i):
        far = part(i, 3)
        r1p_s[i] = far[0:2].astype(BF)
        c_r1p(i).start()
        r1m_s[i] = far[2:4].astype(BF)
        c_r1m(i).start()

    def red_free(i):
        r2p_s[i, 2:4] = part(i, 2)[2:4].astype(BF)
        c_r2p(i, 1).start()
        r2m_s[i, 0:2] = part(i, 1)[0:2].astype(BF)
        c_r2m(i, 0).start()

    def red_mid(i):
        c_r1p(i).wait_recv()
        r2p_s[i, 0:2] = (part(i, 2)[0:2] + r1p_r[i].astype(F32)).astype(BF)
        c_r2p(i, 0).start()
        c_r1m(i).wait_recv()
        r2m_s[i, 2:4] = (part(i, 1)[2:4] + r1m_r[i].astype(F32)).astype(BF)
        c_r2m(i, 1).start()

    def red_end(i):
        landed(r2p_r.at[0:2], I_R2 + i)
        return part(i, 0) + r2p_r[i].astype(F32) + r2m_r[i].astype(F32)

    def gb_own(j):
        c_gd(j).wait_recv()
        for x_ in (0, 2):
            for e, v in enumerate(gb_pair(x_, near(j), k)):
                v = v + gd_r[j, x_ + e].astype(F32)
                gbf[:, near(j), :, x_ + e] = v.reshape(2, 4, 32, 128)

    def z_part(n, c):
        h_, l_ = zi(n)
        return gbf[h_, l_, c]

    def c_qp(n, c):
        return rc(qp_s.at[n, c], qp_r.at[n, c], I_QP + 4 * n + c - 2 * min(n, 1), O_QP + min(n, 1), to_p["z"])

    def c_qm(n, c):
        return rc(qm_s.at[n, c], qm_r.at[n, c], I_QM + 4 * n + c - 2, O_QM + min(n, 1), to_m["z"])

    def q_send(n, first):
        for c in range(4):
            if in_p(3 - n, c) and in_p(4 - n, c) != first:
                v = z_part(4 - n, c)
                if not first:
                    c_qp(n - 1, c).wait_recv()
                    v = v + qp_r[n - 1, c].astype(F32)
                qp_s[n, c] = v.astype(BF)
                c_qp(n, c).start()
            if in_m(3 - n, c) and in_m(4 - n, c) != first:
                v = z_part(n - 4, c)
                if not first:
                    c_qm(n - 1, c).wait_recv()
                    v = v + qm_r[n - 1, c].astype(F32)
                qm_s[n, c] = v.astype(BF)
                c_qm(n, c).start()

    ga_strip(x2)
    red_first(9)
    for i in (4, 3, 2, 1):
        red_first(i)
    gb_own(0)
    q_send(0, True)
    gb_own(1)
    gb_own(2)
    q_send(1, True)
    gb_own(3)
    ga_strip(xp)
    red_first(8)
    ga_strip(xm)
    red_first(7)
    for i in (9, 4, 8, 7, 3, 2, 1):
        red_free(i)
    ga_strip(x)
    red_first(6)
    red_free(6)
    red_mid(9)
    red_mid(4)
    q_send(1, False)
    red_mid(8)
    red_mid(3)
    red_mid(7)
    red_mid(2)

    def c_lx(j):
        return rc(lt1, lx.at[x], I_LX, O_LX, dev((xm, xp, x2)[j], y, z, k))

    def c_ly(j):
        return rc(lt2, ly.at[y], I_LY, O_LY, dev(x, (ym, yp, y2)[j], z, k))

    def c_lz(j):
        return rc(lt3, lz.at[z], I_LZ, O_LZ, pillar(j + 1, k)[1])

    c_lk.wait_recv()
    l1 = lk[0] + lk[1]
    lt1[...] = l1
    lx[x] = l1
    for j in range(3):
        c_lx(j).start()

    gaf[y, x2, 0] = red_end(9)
    red_first(0)
    gaf[y2, x, 1] = red_end(4)
    red_first(5)
    red_mid(6)
    red_mid(1)
    q_send(2, False)
    gaf[y, xp, 0] = red_end(8)
    gaf[y, xm, 0] = red_end(7)
    red_free(0)
    gaf[yp, x, 1] = red_end(3)
    gaf[ym, x, 1] = red_end(2)
    red_free(5)
    red_mid(0)
    red_mid(5)
    landed(lx.at[0:3], I_LX)
    l2 = (lx[0] + lx[1]) + (lx[2] + lx[3])
    lt2[...] = l2
    ly[y] = l2
    for j in range(3):
        c_ly(j).start()
    q_send(3, False)
    gaf[y, x, 0] = red_end(6)
    gaf[y, x, 1] = red_end(1)

    def c_ox(t):
        m, to = plane(t)
        return rc(ox_s.at[m], fin_b.at[mb_slot], I_OX, O_OX, to)

    for c in range(4):
        c_qp(3, c).wait_recv()
        c_qm(3, c).wait_recv()
        v = z_part(0, c) + qp_r[3, c].astype(F32) + qm_r[3, c].astype(F32)
        for x_ in range(4):
            ox_s[x_ * 4 + c] = v[x_].astype(BF)
    for t in far_xy:
        c_ox(t).start()
    fin_b[mb_slot] = ox_s[mb_slot]
    landed(ly.at[0:3], I_LY)
    l3 = (ly[0] + ly[1]) + (ly[2] + ly[3])
    lt3[...] = l3
    lz[z] = l3
    for j in range(7):
        c_lz(j).start()

    def c_oz(t, k_):
        s, to = pillar(t, k_)
        return rc(oz_s.at[s, k_], fin_a.at[z, k], I_OZ, O_OZ, to)

    oz_s[0:4] = red_end(0).astype(BF)
    oz_s[4:8] = red_end(5).astype(BF)
    for t, k_ in far_z:
        c_oz(t, k_).start()
    fin_a[z, k] = oz_s[z, k]

    landed(stz.at[0:3], I_SZ)
    st = ((stz[0] + stz[1]) + (stz[2] + stz[3])) / S
    ma_, mb_ = st[0:1], st[2:3]
    inva_ = lax.rsqrt(st[1:2] - ma_ * ma_ + EPS)
    invb_ = lax.rsqrt(st[3:4] - mb_ * mb_ + EPS)
    c_ = (st[4:5] - ma_ * mb_) * (inva_ * invb_)
    d_ = -2.0 * (1.0 - c_)

    landed(lz.at[0:7], I_LZ)
    lall = lz[0]
    for i in range(1, 8):
        lall = lall + lz[i]
    loss_out[0, 0] = jnp.sum(lall[0:1, :]) / F

    landed(bt_loc.at[0:15], I_OX)
    for c in range(4):
        at = slice(c * 128, (c + 1) * 128)
        an = (a_in[:, at].astype(F32) - ma_[:, at]) * inva_[:, at]
        bn = (b_in[:, at].astype(F32) - mb_[:, at]) * invb_[:, at]
        gt = fin_b[4 * c:4 * c + 4].reshape(128, 128).astype(F32).T
        gb_out[:, at] = (invb_[:, at] * (d_[:, at] * (an - c_[:, at] * bn) + gt)).astype(BF)

    landed(bt_loc.at[0:15], I_OZ)
    for c in range(4):
        at = slice(c * 128, (c + 1) * 128)
        an = (a_in[:, at].astype(F32) - ma_[:, at]) * inva_[:, at]
        bn = (b_in[:, at].astype(F32) - mb_[:, at]) * invb_[:, at]
        gt = fin_a[2 * c:2 * c + 2].reshape(128, 128).astype(F32).T
        ga_out[:, at] = (inva_[:, at] * (d_[:, at] * (bn - c_[:, at] * an) + gt)).astype(BF)

    for e in (O_V1, O_W1, O_OX, O_OZ):
        left(bt_loc.at[0:15], e)
    left(st1, O_SK)
    left(stx.at[0:3], O_SX)
    left(stz.at[0:3], O_SZ)
    left(lt0, O_LK)
    left(lx.at[0:3], O_LX)
    left(ly.at[0:3], O_LY)
    left(lz.at[0:7], O_LZ)
    for e in (O_GP, O_GM, O_R2P, O_R2M):
        left(r2p_s, e)
    for e in (O_GPF, O_GMF, O_R1P, O_R1M):
        left(r1p_s, e)
    for e in (O_WD, O_GD):
        left(gd_s, e)
    for e in (O_ZP, O_ZM, O_QP + 1, O_QM + 1):
        left(qp_s.at[0:3], e)
    for e in (O_ZP + 1, O_ZM + 1, O_QP, O_QM):
        left(qp_s.at[0, 0:2], e)


def shards(view_a, view_b):
    vm = pltpu.VMEM
    block = jax.ShapeDtypeStruct(view_a.shape, BF)
    ga, gb, loss = pl.pallas_call(
        kernel,
        out_shape=(block, block, jax.ShapeDtypeStruct((1, 1), F32)),
        in_specs=[pl.BlockSpec(memory_space=pltpu.HBM)] * 2,
        out_specs=(
            pl.BlockSpec(memory_space=vm),
            pl.BlockSpec(memory_space=vm),
            pl.BlockSpec(memory_space=pltpu.SMEM),
        ),
        scratch_shapes=[
            vm((128, 512), BF), vm((128, 512), BF),
            vm((8, 2, 32, 128), BF), vm((16, 32, 128), BF),
            vm((4, 4, 2, 4, 2, 32, 128), BF),
            vm((2, 4, 2, 4, 4, 32, 128), BF),
            vm((2, 8, 512), F32), vm((4, 8, 512), F32), vm((4, 8, 512), F32),
            vm((8, 512), F32), vm((8, 512), F32), vm((8, 512), F32),
            *[vm((256, 128), F32)] * 4,
            vm((256, 256), F32), vm((256, 256), BF), vm((256, 256), BF),
            vm((256, 128), F32),
            vm((4, 4, 2, 4, 2, 32, 128), F32),
            vm((4, 4, 256, 128), BF), vm((4, 4, 256, 128), BF),
            vm((2, 4, 4, 4, 32, 128), F32),
            *[vm((10, 2, 2, 32, 128), BF)] * 4,
            *[vm((10, 4, 2, 32, 128), BF)] * 4,
            *[vm((4, 4, 4, 32, 128), BF)] * 4,
            vm((8, 2, 32, 128), BF), vm((8, 2, 32, 128), BF),
            vm((16, 32, 128), BF), vm((16, 32, 128), BF),
            *[vm((8, 128), F32)] * 4,
            vm((2, 8, 128), F32), vm((4, 8, 128), F32), vm((4, 8, 128), F32), vm((8, 8, 128), F32),
            pltpu.SemaphoreType.DMA((N_SEND,)),
            pltpu.SemaphoreType.DMA((N_RECV,)),
            pltpu.SemaphoreType.DMA((2,)),
        ],
        compiler_params=pltpu.CompilerParams(
            collective_id=0, has_side_effects=True, vmem_limit_bytes=56 * 1024 * 1024
        ),
    )(view_a, view_b)
    return ga, gb, loss.reshape(())


def solution(mesh):
    return jax.shard_map(
        shards,
        mesh=mesh,
        in_specs=(P("dp", "feat"), P("dp", "feat")),
        out_specs=(P("dp", "feat"), P("dp", "feat"), P()),
        check_vma=False,
    )
```

```python
import jax
import jax.numpy as jnp
from jax import lax
from jax.experimental import pallas as pl
from jax.experimental.pallas import tpu as pltpu
from jax.sharding import PartitionSpec as P

F = 4096
S = 4096
EPS = 1e-05
LAMBDA = 0.0051
MESH = pl.DeviceIdType.MESH
BF = jnp.bfloat16
F32 = jnp.float32


class Slots:
    def __init__(self):
        self.used = 0

    def take(self, n):
        first = self.used
        self.used += n
        return first


SEM = Slots()
I_V1, I_W1, I_SK, I_SX, I_SZ, I_OZ, I_OX, I_LK, I_LX, I_LY, I_LZ = (SEM.take(1) for _ in range(11))
I_GP, I_GM, I_GF = (SEM.take(10) for _ in range(3))
I_ZP, I_ZM = (SEM.take(14) for _ in range(2))
I_WD = SEM.take(8)
I_GD = SEM.take(4)
I_R1P, I_R1M, I_R2 = (SEM.take(10) for _ in range(3))
I_QP, I_QM = (SEM.take(14) for _ in range(2))
N_RECV = SEM.used
OUT = Slots()
(O_V1, O_W1, O_SK, O_SX, O_SZ, O_OZ, O_OX, O_LK, O_LX, O_LY, O_LZ,
 O_GP, O_GM, O_GPF, O_GMF, O_WD, O_GD, O_R1P, O_R1M, O_R2P, O_R2M) = (OUT.take(1) for _ in range(21))
O_ZP, O_ZM, O_QP, O_QM = (OUT.take(2) for _ in range(4))
N_SEND = OUT.used


def kernel(
    a_hbm, b_hbm, ga_out, gb_out, loss_out,
    a_in, b_in, at_loc, bt_loc, va, vb, stk, stx, stz, st1, st2, st3,
    asum, asq, bsum, bsq, raw, g1t, g2, cols,
    gaf, gd_s, gd_r, gbf, r1p_s, r1m_s, r1p_r, r1m_r, r2p_s, r2m_s, r2p_r, r2m_r,
    qp_s, qm_s, qp_r, qm_r, oz_s, fin_a, ox_s, fin_b,
    lt0, lt1, lt2, lt3, lk, lx, ly, lz, ssem, rsem, isem,
):
    dp = lax.axis_index("dp")
    ft = lax.axis_index("feat")
    k = lax.rem(dp, 2)
    x = lax.rem(lax.div(dp, 2), 4)
    zl = lax.div(dp, 8)
    y, zh = lax.div(ft, 2), lax.rem(ft, 2)
    z = zh * 4 + zl
    o = 1 - k
    mb_slot = x * 4 + y
    xs = (x, lax.rem(x + 3, 4), lax.rem(x + 1, 4), lax.rem(x + 2, 4))
    ys = (y, lax.rem(y + 3, 4), lax.rem(y + 1, 4), lax.rem(y + 2, 4))
    _, xm, xp, x2 = xs
    _, ym, yp, y2 = ys

    def dev(x_, y_, z_, k_):
        return (lax.rem(z_, 4) * 8 + x_ * 2 + k_, y_ * 2 + lax.div(z_, 4))

    def zi(n):
        s = lax.rem(z + (n + 8), 8)
        return lax.div(s, 4), lax.rem(s, 4)

    def rc(src, dst, i, e, to):
        return pltpu.make_async_remote_copy(
            src_ref=src, dst_ref=dst, send_sem=ssem.at[e], recv_sem=rsem.at[i],
            device_id=to, device_id_type=MESH,
        )

    def landed(ref, i):
        rc(ref, ref, i, 0, partner).wait_recv()

    def left(ref, e):
        rc(ref, ref, 0, e, partner).wait_send()

    partner = dev(x, y, z, o)
    to_p = {"x": dev(xp, y, z, k), "y": dev(x, yp, z, k), "z": dev(x, y, lax.rem(z + 1, 8), k)}
    to_m = {"x": dev(xm, y, z, k), "y": dev(x, ym, z, k), "z": dev(x, y, lax.rem(z + 7, 8), k)}

    barrier = pltpu.get_barrier_semaphore()

    def greet(to):
        pl.semaphore_signal(barrier, inc=1, device_id=to, device_id_type=MESH)

    def plane(t):
        m = lax.rem(mb_slot + t, 16)
        return m, dev(lax.div(m, 4), lax.rem(m, 4), z, k)

    def pillar(t, k_):
        s = lax.rem(z + t, 8)
        return s, dev(x, y, s, k_)

    load_a = pltpu.make_async_copy(a_hbm, a_in, isem.at[0])
    load_b = pltpu.make_async_copy(b_hbm, b_in, isem.at[1])
    load_a.start()
    load_b.start()

    far_z = [(t, k_) for t in (4, 3, 5, 2, 6, 1, 7) for k_ in (k, o)] + [(0, o)]
    far_xy = (10, 14, 6, 9, 11, 2, 8, 5, 13, 7, 15, 3, 12, 4, 1)

    for t, k_ in far_z:
        greet(pillar(t, k_)[1])
    for t in far_xy:
        greet(plane(t)[1])

    load_a.wait()
    for c in range(4):
        part = slice(c * 128, (c + 1) * 128)
        at_loc[2 * c:2 * c + 2] = a_in[:, part].astype(F32).T.astype(BF).reshape(2, 2, 32, 128)
    va[y, x, zh, zl, k] = at_loc[z, k]
    pl.semaphore_wait(barrier, 30)

    def c_v1(t, k_):
        s, to = pillar(t, k_)
        return rc(at_loc.at[s, k_], va.at[y, x, zh, zl, k], I_V1, O_V1, to)

    def c_w1(t):
        m, to = plane(t)
        return rc(bt_loc.at[m], vb.at[zh, zl, k, y, x], I_W1, O_W1, to)

    for t, k_ in far_z:
        c_v1(t, k_).start()
    load_b.wait()
    for c in range(4):
        part = slice(c * 128, (c + 1) * 128)
        bt_loc[4 * c:4 * c + 4] = b_in[:, part].astype(F32).T.astype(BF).reshape(4, 32, 128)
    for t in far_xy:
        c_w1(t).start()
    vb[zh, zl, k, y, x] = bt_loc[mb_slot]

    af, bf = a_in[...].astype(F32), b_in[...].astype(F32)
    st1[...] = jnp.zeros_like(st1)
    for i, v in enumerate((af, af * af, bf, bf * bf, af * bf)):
        st1[i:i + 1, :] = jnp.sum(v, axis=0, keepdims=True)
    stk[k] = st1[...]
    c_sk = rc(st1, stk.at[k], I_SK, O_SK, partner)
    c_sk.start()

    def ring_blocks(i):
        if i == 0:
            return "x", [va.at[y, xs[j], 0] for j in range(4)]
        if i < 5:
            return "x", [va.at[ys[i - 1], xs[j], 1] for j in range(4)]
        if i == 5:
            return "y", [va.at[ys[j], x, 1] for j in range(4)]
        return "y", [va.at[ys[j], xs[i - 6], 0] for j in range(4)]

    def c_gp(i):
        axis, b = ring_blocks(i)
        return rc(b[0], b[0], I_GP + i, O_GP, to_p[axis])

    def c_gm(i):
        axis, b = ring_blocks(i)
        return rc(b[0], b[0], I_GM + i, O_GM, to_m[axis])

    def c_gpf(i):
        axis, b = ring_blocks(i)
        return rc(b[1].at[0:2], b[1].at[0:2], I_GF + i, O_GPF, to_p[axis])

    def c_gmf(i):
        axis, b = ring_blocks(i)
        return rc(b[2].at[2:4], b[2].at[2:4], I_GF + i, O_GMF, to_m[axis])

    def ring_start(i):
        c_gp(i).start()
        c_gm(i).start()

    def ring_mid(i, then=None):
        c_gp(i).wait_recv()
        c_gpf(i).start()
        if then is not None:
            ring_start(then + 1)
        c_gm(i).wait_recv()
        c_gmf(i).start()
        if then is not None:
            ring_start(then + 2)

    def ring_end(i, then=None):
        landed(ring_blocks(i)[1][3], I_GF + i)
        if then is not None:
            ring_start(then + 3)

    def z_chunk(n, c):
        h_, l_ = zi(n)
        return vb.at[h_, l_, k, c]

    def c_zp(n, c):
        ref = z_chunk(-n, c)
        return rc(ref, ref, I_ZP + 4 * n + c, O_ZP + n // 3, to_p["z"])

    def c_zm(n, c):
        ref = z_chunk(n, c)
        return rc(ref, ref, I_ZM + 4 * n + c - 2 * (n // 3), O_ZM + n // 3, to_m["z"])

    def c_wd(n, c):
        ref = z_chunk(n, c)
        return rc(ref, ref, I_WD + n % 8, O_WD, partner)

    def in_p(n, c):
        return n < 3 or (n == 3 and c < 2)

    def in_m(n, c):
        return n < 3 or (n == 3 and c >= 2)

    def z_step(n):
        for c in range(4):
            if in_p(n, c):
                c_zp(n, c).wait_recv()
                if in_p(n + 1, c):
                    c_zp(n + 1, c).start()
                c_wd(-(n + 1), c).start()
            if in_m(n, c):
                c_zm(n, c).wait_recv()
                if in_m(n + 1, c):
                    c_zm(n + 1, c).start()
                c_wd(n + 1, c).start()

    landed(bt_loc.at[0:15], I_V1)
    ring_start(0)
    ring_start(5)
    ring_start(1)
    ring_start(6)
    landed(bt_loc.at[0:15], I_W1)
    for c in range(4):
        c_zp(0, c).start()
        c_zm(0, c).start()
    for c in range(4):
        c_wd(0, c).start()

    c_sk.wait_recv()
    sk = stk[0] + stk[1]
    st2[...] = sk
    stx[x] = sk

    def c_sx(j):
        return rc(st2, stx.at[x], I_SX, O_SX, dev((xm, xp, x2)[j], y, z, k))

    for j in range(3):
        c_sx(j).start()

    ring_mid(0, then=6)
    ring_mid(5, then=1)
    z_step(0)
    ring_end(0, then=6)
    ring_end(5, then=1)

    landed(stx.at[0:3], I_SX)
    sx = (stx[0] + stx[1]) + (stx[2] + stx[3])
    st3[...] = sx
    stz[zl] = sx

    def c_sz(j):
        l_ = lax.rem(zl + (j + 1), 4)
        return rc(st3, stz.at[zl], I_SZ, O_SZ, dev(x, y, zh * 4 + l_, k))

    for j in range(3):
        c_sz(j).start()

    for ref in (asum, asq, bsum, bsq, raw):
        ref[...] = jnp.zeros_like(ref)

    def va_at(x_, l_, kk):
        return va[:, x_, :, l_, kk].reshape(256, 128)

    def vb_at(x_, l_, kk):
        return vb[:, l_, kk, :, x_].reshape(256, 128)

    def near(j):
        return lax.rem(zl + (0, 1, 3, 2)[j], 4)

    def corr(j):
        l_ = near(j)

        pairs = [(x_, kk) for x_ in range(4) for kk in (0, 1)]
        a_, b_ = ([f(x_, l_, kk) for x_, kk in pairs] for f in (va_at, vb_at))
        raw[...] += lax.dot_general(
            jnp.concatenate(b_, axis=1), jnp.concatenate(a_, axis=1),
            (((1,), (1,)), ((), ())), preferred_element_type=F32,
        )
        for f, s_, q_ in ((va_at, asum, asq), (vb_at, bsum, bsq)):
            for h in range(4):
                at = slice(h * 64, h * 64 + 64)
                v = [f(x_, l_, kk)[at].astype(F32) for x_, kk in pairs]
                s_[at, :] += sum(v[1:], v[0])
                q_[at, :] += sum((u * u for u in v[1:]), v[0] * v[0])

    def from_core(n):
        h_, l_ = zi(n)
        landed(vb.at[h_, l_, o], I_WD + n % 8)

    ring_mid(1)
    ring_mid(6)
    z_step(1)
    ring_mid(2)
    ring_mid(7)
    ring_mid(3)
    ring_mid(8)
    z_step(2)
    ring_mid(4)
    ring_mid(9)
    for i in (1, 6, 2, 7, 3, 8, 4, 9):
        ring_end(i)
    z_step(3)
    from_core(2)
    from_core(-2)
    corr(3)
    from_core(1)
    from_core(-3)
    corr(1)
    from_core(-1)
    from_core(3)
    corr(2)
    from_core(0)
    from_core(4)
    corr(0)
    row = lax.broadcasted_iota(jnp.int32, (256, 256), 0)
    col = lax.broadcasted_iota(jnp.int32, (256, 256), 1)
    zero = jnp.zeros((256, 256), F32)
    eye = row == col

    def to_row(v):
        return jnp.sum(jnp.where(eye, v, zero), axis=0, keepdims=True)

    def to_col(v):
        return jnp.sum(jnp.where(eye, v, zero), axis=1, keepdims=True)

    ma = jnp.sum(asum[...], axis=1, keepdims=True) / S
    inva = lax.rsqrt(jnp.sum(asq[...], axis=1, keepdims=True) / S - ma * ma + EPS)
    mb = jnp.sum(bsum[...], axis=1, keepdims=True) / S
    invb = lax.rsqrt(jnp.sum(bsq[...], axis=1, keepdims=True) / S - mb * mb + EPS)
    ma_r, inva_r = to_row(ma), to_row(inva)
    ct = (raw[...] / S - mb * ma_r) * (invb * inva_r)

    def bits(v, shift, mask):
        return lax.bitwise_and(lax.shift_right_logical(v, shift), mask)

    j_id = (bits(row, 5, 3) * 2 + bits(row, 7, 1)) * 512 + mb_slot * 32 + bits(row, 0, 31)
    i_id = bits(col, 5, 7) * 512 + (z * 2 + k) * 32 + bits(col, 0, 31)
    unit = j_id == i_id
    g = jnp.where(unit, zero, (2.0 * LAMBDA) * ct)
    g1 = (invb * g).astype(BF).astype(F32)
    g1t[...] = g1.T.astype(BF)
    g2v = (g * inva_r).astype(BF)
    g2[...] = g2v
    gc = g * ct
    ua = inva * to_col(jnp.sum(gc, axis=0, keepdims=True))
    ub = invb * jnp.sum(gc, axis=1, keepdims=True)
    cols[:, 0:1] = ua
    cols[:, 1:2] = to_col(jnp.sum(g1 * mb, axis=0, keepdims=True)) - ma * ua
    cols[:, 2:3] = ub
    cols[:, 3:4] = jnp.sum(g2v.astype(F32) * ma_r, axis=1, keepdims=True) - mb * ub
    lv = jnp.sum(
        jnp.where(unit, (1.0 - ct) * (1.0 - ct), LAMBDA * ct * ct), axis=0, keepdims=True
    )
    l0 = jnp.broadcast_to(lv[:, 0:128] + lv[:, 128:256], (8, 128))
    lt0[...] = l0
    lk[k] = l0
    c_lk = rc(lt0, lk.at[k], I_LK, O_LK, partner)
    c_lk.start()

    def gb_pair(x_, l_, kk):
        a0, a1 = va_at(x_, l_, kk), va_at(x_ + 1, l_, kk)
        prod = jnp.dot(g2[...], jnp.concatenate([a0, a1], axis=1), preferred_element_type=F32)
        return [
            prod[:, e * 128:(e + 1) * 128]
            - vb_at(x_ + e, l_, kk).astype(F32) * cols[:, 2:3] - cols[:, 3:4]
            for e in (0, 1)
        ]

    def c_gd(j):
        return rc(gd_s.at[j], gd_r.at[j], I_GD + j, O_GD, partner)

    for j in range(4):
        for x_ in (0, 2):
            for e, v in enumerate(gb_pair(x_, near(j), o)):
                gd_s[j, x_ + e] = v.astype(BF)
        c_gd(j).start()

    def ga_strip(x_):
        @pl.loop(0, 4)
        def _(l_):
            b01 = jnp.concatenate([vb_at(x_, l_, 0), vb_at(x_, l_, 1)], axis=1)
            prod = jnp.dot(g1t[...], b01, preferred_element_type=F32)
            for e in (0, 1):
                gaf[:, x_, :, l_, e] = (
                    prod[:, e * 128:(e + 1) * 128]
                    - va_at(x_, l_, e).astype(F32) * cols[:, 0:1] - cols[:, 1:2]
                ).reshape(4, 2, 32, 128)

    def axis_of(i):
        return "x" if i < 5 else "y"

    def part(i, j):
        if i == 0:
            return gaf[y, xs[j], 0]
        if i < 5:
            return gaf[ys[i - 1], xs[j], 1]
        if i == 5:
            return gaf[ys[j], x, 1]
        return gaf[ys[j], xs[i - 6], 0]

    def c_r1p(i):
        return rc(r1p_s.at[i], r1p_r.at[i], I_R1P + i, O_R1P, to_p[axis_of(i)])

    def c_r1m(i):
        return rc(r1m_s.at[i], r1m_r.at[i], I_R1M + i, O_R1M, to_m[axis_of(i)])

    def c_r2p(i, h):
        at = slice(2 * h, 2 * h + 2)
        return rc(r2p_s.at[i, at], r2p_r.at[i, at], I_R2 + i, O_R2P, to_p[axis_of(i)])

    def c_r2m(i, h):
        at = slice(2 * h, 2 * h + 2)
        return rc(r2m_s.at[i, at], r2m_r.at[i, at], I_R2 + i, O_R2M, to_m[axis_of(i)])

    def red_first(i):
        far = part(i, 3)
        r1p_s[i] = far[0:2].astype(BF)
        c_r1p(i).start()
        r1m_s[i] = far[2:4].astype(BF)
        c_r1m(i).start()

    def red_free(i):
        r2p_s[i, 2:4] = part(i, 2)[2:4].astype(BF)
        c_r2p(i, 1).start()
        r2m_s[i, 0:2] = part(i, 1)[0:2].astype(BF)
        c_r2m(i, 0).start()

    def red_mid(i):
        c_r1p(i).wait_recv()
        r2p_s[i, 0:2] = (part(i, 2)[0:2] + r1p_r[i].astype(F32)).astype(BF)
        c_r2p(i, 0).start()
        c_r1m(i).wait_recv()
        r2m_s[i, 2:4] = (part(i, 1)[2:4] + r1m_r[i].astype(F32)).astype(BF)
        c_r2m(i, 1).start()

    def red_end(i):
        landed(r2p_r.at[0:2], I_R2 + i)
        return part(i, 0) + r2p_r[i].astype(F32) + r2m_r[i].astype(F32)

    def gb_own(j):
        c_gd(j).wait_recv()
        for x_ in (0, 2):
            for e, v in enumerate(gb_pair(x_, near(j), k)):
                v = v + gd_r[j, x_ + e].astype(F32)
                gbf[:, near(j), :, x_ + e] = v.reshape(2, 4, 32, 128)

    def z_part(n, c):
        h_, l_ = zi(n)
        return gbf[h_, l_, c]

    def c_qp(n, c):
        return rc(qp_s.at[n, c], qp_r.at[n, c], I_QP + 4 * n + c - 2 * min(n, 1), O_QP + min(n, 1), to_p["z"])

    def c_qm(n, c):
        return rc(qm_s.at[n, c], qm_r.at[n, c], I_QM + 4 * n + c - 2, O_QM + min(n, 1), to_m["z"])

    def q_send(n, first):
        for c in range(4):
            if in_p(3 - n, c) and in_p(4 - n, c) != first:
                v = z_part(4 - n, c)
                if not first:
                    c_qp(n - 1, c).wait_recv()
                    v = v + qp_r[n - 1, c].astype(F32)
                qp_s[n, c] = v.astype(BF)
                c_qp(n, c).start()
            if in_m(3 - n, c) and in_m(4 - n, c) != first:
                v = z_part(n - 4, c)
                if not first:
                    c_qm(n - 1, c).wait_recv()
                    v = v + qm_r[n - 1, c].astype(F32)
                qm_s[n, c] = v.astype(BF)
                c_qm(n, c).start()

    gb_own(0)
    q_send(0, True)
    ga_strip(x2)
    for i in (9, 4, 3, 2, 1):
        red_first(i)
    gb_own(1)
    gb_own(2)
    q_send(1, True)
    ga_strip(xp)
    red_first(8)
    ga_strip(xm)
    red_first(7)
    red_free(9)
    red_free(4)
    gb_own(3)
    q_send(1, False)
    red_mid(9)
    red_mid(4)
    for i in (8, 7, 3, 2, 1):
        red_free(i)
    ga_strip(x)
    red_first(6)
    red_free(6)
    for i in (8, 3):
        red_mid(i)
    q_send(2, False)
    for i in (7, 2):
        red_mid(i)

    def c_lx(j):
        return rc(lt1, lx.at[x], I_LX, O_LX, dev((xm, xp, x2)[j], y, z, k))

    def c_ly(j):
        return rc(lt2, ly.at[y], I_LY, O_LY, dev(x, (ym, yp, y2)[j], z, k))

    def c_lz(j):
        return rc(lt3, lz.at[z], I_LZ, O_LZ, pillar(j + 1, k)[1])

    c_lk.wait_recv()
    l1 = lk[0] + lk[1]
    lt1[...] = l1
    lx[x] = l1
    for j in range(3):
        c_lx(j).start()

    gaf[y, x2, 0] = red_end(9)
    red_first(0)
    gaf[y2, x, 1] = red_end(4)
    red_first(5)
    red_mid(6)
    red_mid(1)
    gaf[y, xp, 0] = red_end(8)
    gaf[y, xm, 0] = red_end(7)
    red_free(0)
    gaf[yp, x, 1] = red_end(3)
    gaf[ym, x, 1] = red_end(2)
    red_free(5)
    landed(lx.at[0:3], I_LX)
    l2 = (lx[0] + lx[1]) + (lx[2] + lx[3])
    lt2[...] = l2
    ly[y] = l2
    for j in range(3):
        c_ly(j).start()
    q_send(3, False)
    red_mid(0)
    red_mid(5)
    gaf[y, x, 0] = red_end(6)
    gaf[y, x, 1] = red_end(1)

    def c_ox(x_, y_):
        m = x_ * 4 + y_
        return rc(ox_s.at[m], fin_b.at[mb_slot], I_OX, O_OX, dev(x_, y_, z, k))

    for c in range(4):
        c_qp(3, c).wait_recv()
        c_qm(3, c).wait_recv()
        v = z_part(0, c) + qp_r[3, c].astype(F32) + qm_r[3, c].astype(F32)
        for x_ in range(4):
            ox_s[x_ * 4 + c] = v[x_].astype(BF)
        for x_ in (x2, xm, xp):
            c_ox(x_, c).start()

        @pl.when(y != c)
        def _():
            c_ox(x, c).start()

    fin_b[mb_slot] = ox_s[mb_slot]
    landed(ly.at[0:3], I_LY)
    l3 = (ly[0] + ly[1]) + (ly[2] + ly[3])
    lt3[...] = l3
    lz[z] = l3
    for j in range(7):
        c_lz(j).start()

    def c_oz(s, k_):
        return rc(oz_s.at[s, k_], fin_a.at[z, k], I_OZ, O_OZ, dev(x, y, s, k_))

    for h, i in ((0, 0), (1, 5)):
        oz_s[4 * h:4 * h + 4] = red_end(i).astype(BF)
        for d in (2, 3, 1, 0):
            s = 4 * h + lax.rem(zl + d, 4)
            c_oz(s, o).start()
            if d:
                c_oz(s, k).start()
            else:
                @pl.when(zh != h)
                def _():
                    c_oz(s, k).start()

    fin_a[z, k] = oz_s[z, k]

    landed(stz.at[0:3], I_SZ)
    st = ((stz[0] + stz[1]) + (stz[2] + stz[3])) / S
    ma_, mb_ = st[0:1], st[2:3]
    inva_ = lax.rsqrt(st[1:2] - ma_ * ma_ + EPS)
    invb_ = lax.rsqrt(st[3:4] - mb_ * mb_ + EPS)
    c_ = (st[4:5] - ma_ * mb_) * (inva_ * invb_)
    d_ = -2.0 * (1.0 - c_)

    landed(lz.at[0:7], I_LZ)
    lall = lz[0]
    for i in range(1, 8):
        lall = lall + lz[i]
    loss_out[0, 0] = jnp.sum(lall[0:1, :]) / F

    landed(bt_loc.at[0:15], I_OX)
    for c in range(4):
        at = slice(c * 128, (c + 1) * 128)
        an = (a_in[:, at].astype(F32) - ma_[:, at]) * inva_[:, at]
        bn = (b_in[:, at].astype(F32) - mb_[:, at]) * invb_[:, at]
        gt = fin_b[4 * c:4 * c + 4].reshape(128, 128).astype(F32).T
        gb_out[:, at] = (invb_[:, at] * (d_[:, at] * (an - c_[:, at] * bn) + gt)).astype(BF)

    landed(bt_loc.at[0:15], I_OZ)
    for c in range(4):
        at = slice(c * 128, (c + 1) * 128)
        an = (a_in[:, at].astype(F32) - ma_[:, at]) * inva_[:, at]
        bn = (b_in[:, at].astype(F32) - mb_[:, at]) * invb_[:, at]
        gt = fin_a[2 * c:2 * c + 2].reshape(128, 128).astype(F32).T
        ga_out[:, at] = (inva_[:, at] * (d_[:, at] * (bn - c_[:, at] * an) + gt)).astype(BF)

    for e in (O_V1, O_W1, O_OX, O_OZ):
        left(bt_loc.at[0:15], e)
    left(st1, O_SK)
    left(stx.at[0:3], O_SX)
    left(stz.at[0:3], O_SZ)
    left(lt0, O_LK)
    left(lx.at[0:3], O_LX)
    left(ly.at[0:3], O_LY)
    left(lz.at[0:7], O_LZ)
    for e in (O_GP, O_GM, O_R2P, O_R2M):
        left(r2p_s, e)
    for e in (O_GPF, O_GMF, O_R1P, O_R1M):
        left(r1p_s, e)
    for e in (O_WD, O_GD):
        left(gd_s, e)
    for e in (O_ZP, O_ZM, O_QP + 1, O_QM + 1):
        left(qp_s.at[0:3], e)
    for e in (O_ZP + 1, O_ZM + 1, O_QP, O_QM):
        left(qp_s.at[0, 0:2], e)


def shards(view_a, view_b):
    vm = pltpu.VMEM
    block = jax.ShapeDtypeStruct(view_a.shape, BF)
    ga, gb, loss = pl.pallas_call(
        kernel,
        out_shape=(block, block, jax.ShapeDtypeStruct((1, 1), F32)),
        in_specs=[pl.BlockSpec(memory_space=pltpu.HBM)] * 2,
        out_specs=(
            pl.BlockSpec(memory_space=vm),
            pl.BlockSpec(memory_space=vm),
            pl.BlockSpec(memory_space=pltpu.SMEM),
        ),
        scratch_shapes=[
            vm((128, 512), BF), vm((128, 512), BF),
            vm((8, 2, 32, 128), BF), vm((16, 32, 128), BF),
            vm((4, 4, 2, 4, 2, 32, 128), BF),
            vm((2, 4, 2, 4, 4, 32, 128), BF),
            vm((2, 8, 512), F32), vm((4, 8, 512), F32), vm((4, 8, 512), F32),
            vm((8, 512), F32), vm((8, 512), F32), vm((8, 512), F32),
            *[vm((256, 128), F32)] * 4,
            vm((256, 256), F32), vm((256, 256), BF), vm((256, 256), BF),
            vm((256, 128), F32),
            vm((4, 4, 2, 4, 2, 32, 128), F32),
            vm((4, 4, 256, 128), BF), vm((4, 4, 256, 128), BF),
            vm((2, 4, 4, 4, 32, 128), F32),
            *[vm((10, 2, 2, 32, 128), BF)] * 4,
            *[vm((10, 4, 2, 32, 128), BF)] * 4,
            *[vm((4, 4, 4, 32, 128), BF)] * 4,
            vm((8, 2, 32, 128), BF), vm((8, 2, 32, 128), BF),
            vm((16, 32, 128), BF), vm((16, 32, 128), BF),
            *[vm((8, 128), F32)] * 4,
            vm((2, 8, 128), F32), vm((4, 8, 128), F32), vm((4, 8, 128), F32), vm((8, 8, 128), F32),
            pltpu.SemaphoreType.DMA((N_SEND,)),
            pltpu.SemaphoreType.DMA((N_RECV,)),
            pltpu.SemaphoreType.DMA((2,)),
        ],
        compiler_params=pltpu.CompilerParams(
            collective_id=0, has_side_effects=True, vmem_limit_bytes=56 * 1024 * 1024
        ),
    )(view_a, view_b)
    return ga, gb, loss.reshape(())


def solution(mesh):
    return jax.shard_map(
        shards,
        mesh=mesh,
        in_specs=(P("dp", "feat"), P("dp", "feat")),
        out_specs=(P("dp", "feat"), P("dp", "feat"), P()),
        check_vma=False,
    )
```
